128 devices in a mesh: dp: 64 (over y, x, z_hi, core), mp: 2 (over z_lo).
Axes of the slice: x: 4, y: 4, z: 4 (z_hi: 2, z_lo: 2; z = z_hi * 2 + z_lo), core: 2. Of those that a mesh axis runs over, the one named last changes fastest.
Arguments:
- pooled_grad: bfloat16 [16384, 128, 128], P(('dp', 'mp')), may hold values from -6 to 6
- bag_lengths: int32 [16384, 128], P(('dp', 'mp')), may hold values from 1 to 4
- bag_rows: int32 [16384, 128, 4], P(('dp', 'mp')), may hold values from 0 to 2047
- table_rows: float32 [128, 2048, 128], P('dp', 'mp'), may hold values from -6 to 6
- row_accum: float32 [128, 2048], P('dp', 'mp'), may hold values from 0.01 to 1
- dense_input: bfloat16 [16384, 1024], P(('dp', 'mp')), may hold values from -6 to 6
- dense_cotangent: bfloat16 [16384, 1024], P(('dp', 'mp')), may hold values from -0.046875 to 0.046875
Outputs:
- new_rows: float32 [128, 2048, 128], P('dp', 'mp')
- new_accum: float32 [128, 2048], P('dp', 'mp')
- dense_grad: float32 [1024, 1024], replicated
The draws below stay inside these ranges and needn't reach their ends.
Inputs may be any that keep to these rules, and one draw needn't show every extreme that they name: `bag_rows`: a row number of the whole table.
All inputs are finite; a program needn't handle non-finite values.
Results may differ from the reference program's by a relative error of at most 0.0003.
Values may be sent and summed in bfloat16 or wider, within the bound.
No kernel may reach another device: no remote copies, remote signals or barrier semaphores. Data moves between devices by JAX's collectives and lax.ppermute only.
A program may use at most 128 MiB of HBM per device.

```python
import math
import jax
import jax.numpy as jnp
import numpy as np
from jax import lax

E = 128
D_IN = 1024
D_OUT = 1024
BAG = 4
TABLES = 128
ROWS = 2048
B_ALL = 16384


def plant(drawn, own_key, smallest, top_value):
    index_at = [jax.random.randint(jax.random.fold_in(own_key, axis), (), 0, length) for axis, length in enumerate(drawn.shape)]
    widest = drawn.shape.index(max(drawn.shape))
    beside = index_at[:widest] + [(index_at[widest] + 1) % drawn.shape[widest]] + index_at[widest + 1:]
    return drawn.at[tuple(index_at)].set(smallest).at[tuple(beside)].set(top_value)


def block_scale(own_key, shape, split, least, high):
    gain, own = 1.0, jax.random.fold_in(own_key, 6)
    for position, parts in split:
        draws = jnp.exp(jax.random.uniform(jax.random.fold_in(own, position), (parts,), jnp.float32, least / len(split), high / len(split)))
        gain = gain * jnp.repeat(draws, shape[position] // parts).reshape([-1 if axis == position else 1 for axis in range(len(shape))])
    return gain


def rank_table(number_of, skew):
    loads = [(1 << 20) // math.isqrt(standing ** skew) + 1 for standing in range(1, number_of + 1)]
    scale = 1 + sum(loads) // (1 << 30)
    return np.cumsum(np.array([max(1, weight // scale) for weight in loads]))


def ranked_ids(own_key, dims, amount, skew):
    table = rank_table(amount, skew)
    ticket = jax.random.randint(jax.random.fold_in(own_key, 1), dims, 0, int(table[amount - 1]))
    rank = jnp.searchsorted(jnp.asarray(table, jnp.int32), ticket, side="right")
    return jax.random.permutation(jax.random.fold_in(own_key, 2), amount)[rank].astype(jnp.int32)


def noise(key, dims, deviation, reach, split=(), kind=jnp.bfloat16):
    gain = block_scale(key, dims, split, -0.22, 0.18) if split else 1.0
    result = jax.random.normal(key, dims, jnp.float32) * deviation * gain
    return jnp.minimum(jnp.maximum(result, -reach), reach).astype(kind)


def setup_inputs(seed: int = 0) -> dict:
    keys = jax.random.split(jax.random.key(seed), 8)
    pooled_grad = noise(keys[0], (B_ALL, TABLES, E), 1.0, 6.0, ((0, 128),))
    bag_lengths = plant(jax.random.randint(keys[1], (B_ALL, TABLES), 1, BAG + 1), jax.random.fold_in(keys[1], 1), 1, BAG).astype(jnp.int32)
    bag_rows = plant(ranked_ids(keys[2], (B_ALL, TABLES, BAG), ROWS, 2), jax.random.fold_in(keys[2], 3), 0, ROWS - 1).astype(jnp.int32)
    table_rows = noise(keys[3], (TABLES, ROWS, E), 1.0, 6.0, ((0, 64), (1, 2)), jnp.float32)
    row_accum = jnp.clip(jnp.exp(math.log(1.0) - 4.6051702 * jax.random.uniform(keys[4], (TABLES, ROWS), jnp.float32) ** block_scale(keys[4], (TABLES, ROWS), ((0, 64), (1, 2)), -0.2, 0.2)), 0.01, 1.0)
    dense_input = noise(keys[5], (B_ALL, D_IN), 1.0, 6.0, ((0, 128),))
    dense_cotangent = noise(keys[6], (B_ALL, D_OUT), B_ALL ** -0.5, 0.046875, ((0, 128),))
    return dict(pooled_grad=pooled_grad, bag_lengths=bag_lengths, bag_rows=bag_rows, table_rows=table_rows, row_accum=row_accum, dense_input=dense_input, dense_cotangent=dense_cotangent)


learn_rate = 0.5

def reference(pooled_grad, bag_lengths, bag_rows, table_rows, row_accum, dense_input, dense_cotangent):

    def one_table(table):
        column_grad = lax.dynamic_index_in_dim(pooled_grad, table, 1, keepdims=False)
        lengths = lax.dynamic_index_in_dim(bag_lengths, table, 1, keepdims=False)
        looked = lax.dynamic_index_in_dim(bag_rows, table, 1, keepdims=False)
        active = jnp.arange(BAG, dtype=jnp.int32)[None, :] < lengths[:, None]
        values = jnp.where(active[..., None], column_grad[:, None, :].astype(jnp.float32), jnp.zeros((), jnp.float32))
        values = values.reshape(-1, column_grad.shape[-1])
        return jax.ops.segment_sum(values, looked.reshape(-1).astype(jnp.int32), num_segments=ROWS)
    row_grad = lax.map(one_table, jnp.arange(TABLES, dtype=jnp.int32))
    new_accum = row_accum + lax.optimization_barrier(jnp.mean(row_grad * row_grad, axis=-1))
    new_rows = table_rows - learn_rate * row_grad / jnp.sqrt(new_accum)[..., None]
    dense_grad = lax.dot_general(dense_input, dense_cotangent, (((0,), (0,)), ((), ())), preferred_element_type=jnp.float32)
    return (new_rows, new_accum, dense_grad)
```

```python
import functools

import jax
import jax.numpy as jnp
from jax import lax
from jax.experimental import pallas as pl
from jax.experimental.pallas import tpu as pltpu
from jax.sharding import Mesh, PartitionSpec as P

learn_rate = 0.5
ring = 4
every = ("y", "x", "zh", "c", "zl")
deep = ("zh", "zl")
f32 = jnp.float32
bf16 = jnp.bfloat16


def coded(row):
    size = (128 + (row & 127)) << ((row >> 7) & 7)
    return jnp.where(row >= 1024, -size, size).astype(f32).astype(bf16)


def slot_codes(lengths, looked):
    rows = jnp.transpose(looked, (1, 2, 0))
    count = jnp.transpose(lengths, (1, 0))
    slots = rows.shape[1]
    active = [count > j for j in range(slots)]
    row = [rows[:, j, :] for j in range(slots)]
    codes, weights = [], []
    for j in range(slots):
        first = active[j]
        for i in range(j):
            first = first & (row[i] != row[j])
        weight = jnp.ones_like(count)
        for i in range(j + 1, slots):
            weight = weight + (active[i] & (row[i] == row[j])).astype(jnp.int32)
        codes.append(jnp.where(first, coded(row[j]), jnp.zeros((), bf16)))
        weights.append(weight.astype(f32).astype(bf16))
    return jnp.stack(codes + weights, axis=1)


def pack_kernel(swap_ref, grad_ref, code_ref, out_ref):
    samples = grad_ref.shape[0]
    tables, _, width = code_ref.shape
    for first in range(0, samples, 16):
        block = grad_ref[first : first + 16].reshape(16 * tables, width)
        turned = jnp.dot(swap_ref[...], block, preferred_element_type=f32)
        out_ref[:, first : first + 16, :] = turned.astype(bf16).reshape(tables, 16, width)
    out_ref[:, samples : samples + 8, :] = code_ref[...]


def packed(grads, codes):
    samples, tables, width = grads.shape
    index = jnp.arange(256, dtype=jnp.int32)
    swap = ((index[:, None] % 16 == index[None, :] // 16) & (index[:, None] // 16 == index[None, :] % 16)).astype(bf16)
    return pl.pallas_call(
        pack_kernel,
        grid=(tables // 16,),
        in_specs=[
            pl.BlockSpec((256, 256), lambda i: (0, 0)),
            pl.BlockSpec((samples, 16, width), lambda i: (0, i, 0)),
            pl.BlockSpec((16, 8, width), lambda i: (i, 0, 0)),
        ],
        out_specs=pl.BlockSpec((16, samples + 8, width), lambda i: (i, 0, 0)),
        out_shape=jax.ShapeDtypeStruct((tables, samples + 8, width), bf16),
        cost_estimate=pl.CostEstimate(flops=2 * 256 * samples * tables * width, bytes_accessed=8 << 20, transcendentals=0),
        name="pack",
    )(swap, grads, codes)


group = 4


def sum_kernel(base_ref, code_ref, data_ref, out_ref):
    senders, height, width = data_ref.shape
    samples = height - 8
    rows = out_ref.shape[0]
    base = base_ref[0]

    @pl.when(pl.program_id(0) == 0)
    def _():
        out_ref[...] = jnp.zeros_like(out_ref)

    mine = code_ref[pl.ds(pl.multiple_of(base, rows), rows), :]
    zero = jnp.zeros((), bf16)
    for first in range(0, senders, group):
        hots = []
        values = []
        for k in range(first, first + group):
            info = data_ref[k, samples:height, :]
            hot = jnp.where(mine == info[3:4], info[7:8], zero)
            for j in (2, 1, 0):
                hot = jnp.where(mine == info[j : j + 1], info[4 + j : 5 + j], hot)
            hots.append(hot)
            values.append(data_ref[k, 0:samples, :])
        out_ref[...] += jnp.dot(
            jnp.concatenate(hots, axis=1), jnp.concatenate(values, axis=0), preferred_element_type=f32
        )


def summed(data, codes, base, rows):
    senders, height, width = data.shape
    step = 8
    return pl.pallas_call(
        sum_kernel,
        grid_spec=pltpu.PrefetchScalarGridSpec(
            num_scalar_prefetch=1,
            grid=(senders // step,),
            in_specs=[
                pl.BlockSpec(codes.shape, lambda i, b: (0, 0)),
                pl.BlockSpec((step, height, width), lambda i, b: (i, 0, 0)),
            ],
            out_specs=pl.BlockSpec((rows, width), lambda i, b: (0, 0)),
        ),
        out_shape=jax.ShapeDtypeStruct((rows, width), f32),
        cost_estimate=pl.CostEstimate(flops=2 * senders * 128 * rows * width, bytes_accessed=5 << 20, transcendentals=0),
        name="sum_by_row",
    )(base, codes, data)


def to_next(value, axis, step):
    return lax.ppermute(value, axis, [(i, (i + step) % ring) for i in range(ring)])


def scattered(value, axis, here):
    arrived = [
        to_next(lax.dynamic_index_in_dim(value, (here + step) % ring, 0, keepdims=False), axis, step)
        for step in range(1, ring)
    ]
    own = lax.dynamic_index_in_dim(value, here, 0, keepdims=False)
    return own + arrived[0] + arrived[1] + arrived[2]


def place_kernel(at_ref, *refs):
    out_ref = refs[-1]
    here_y, here_x, here_z, here_c = (at_ref[k] for k in range(4))
    for core in range(2):
        c = here_c if core == 0 else 1 - here_c
        for dy in range(ring):
            y = (here_y + ring - dy) % ring
            piece = refs[core * ring + dy]
            for dx in range(ring):
                x = (here_x + ring - dx) % ring
                left = pl.multiple_of((x % 2) * 512, 512)
                for dz in range(ring):
                    z = (here_z + ring - dz) % ring
                    top = pl.multiple_of((x // 2) * 512 + c * 256 + y * 64 + z * 16, 16)
                    out_ref[pl.ds(top, 16), pl.ds(left, 512)] = piece[dx, dz]


def placed(at, pieces):
    return pl.pallas_call(
        place_kernel,
        in_specs=[pl.BlockSpec(memory_space=pltpu.SMEM)] + [pl.BlockSpec(memory_space=pltpu.VMEM)] * len(pieces),
        out_specs=pl.BlockSpec(memory_space=pltpu.VMEM),
        out_shape=jax.ShapeDtypeStruct((1024, 1024), f32),
        cost_estimate=pl.CostEstimate(flops=3 << 20, bytes_accessed=8 << 20, transcendentals=0),
        name="place",
    )(at, *pieces)


def dense_sum(inputs, cotangents):
    y, x, c = (lax.axis_index(a) for a in ("y", "x", "c"))
    z = lax.axis_index(deep)

    def share(of):
        one = jnp.where(of // 2 == 0, inputs[:, :512], inputs[:, 512:])
        two = jnp.where(of % 2 == 0, cotangents[:, :512], cotangents[:, 512:])
        return jnp.concatenate([one, two], axis=1)

    parts = [share(x)] + [to_next(share((x + step) % ring), "x", step) for step in range(1, ring)]
    both = jnp.concatenate(parts, axis=0)
    local = lax.dot_general(both[:, :512], both[:, 512:], (((0,), (0,)), ((), ())), preferred_element_type=f32)
    halves = local.reshape(2, 256, 512)
    swap = [(0, 1), (1, 0)]
    other = lax.ppermute(lax.dynamic_index_in_dim(halves, 1 - c, 0, keepdims=False), "c", swap)
    total = lax.dynamic_index_in_dim(halves, c, 0, keepdims=False) + other
    total = scattered(total.reshape(ring, 64, 512), "y", y)
    total = scattered(total.reshape(ring, 16, 512), deep, z)
    total = jnp.stack([total] + [to_next(total, deep, step) for step in range(1, ring)])
    total = jnp.stack([total] + [to_next(total, "x", step) for step in range(1, ring)])
    mine = [total] + [to_next(total, "y", step) for step in range(1, ring)]
    theirs = [lax.ppermute(p, "c", swap) for p in mine]
    return placed(jnp.stack([y, x, z, c]).astype(jnp.int32), mine + theirs)


def per_device(
    pooled_grad, bag_lengths, bag_rows, table_rows, row_accum, dense_input, dense_cotangent
):
    tables, rows = row_accum.shape
    dense_grad = dense_sum(dense_input, dense_cotangent)
    outgoing = packed(pooled_grad, slot_codes(bag_lengths, bag_rows))
    data = lax.all_to_all(outgoing, every, split_axis=0, concat_axis=0, tiled=True)
    codes = jnp.broadcast_to(coded(jnp.arange(tables * rows, dtype=jnp.int32))[:, None], (tables * rows, 128))
    half = lax.axis_index("zl").astype(jnp.int32)
    theirs = summed(data, codes, ((1 - half) * rows)[None], rows)
    arrived = lax.ppermute(theirs, "zl", [(0, 1), (1, 0)])
    own = summed(data, codes, (half * rows)[None], rows)
    row_grad = jnp.where(half == 0, jnp.stack([own, arrived]), jnp.stack([arrived, own]))
    new_accum = row_accum + jnp.mean(row_grad * row_grad, axis=-1)
    new_rows = table_rows - learn_rate * row_grad / jnp.sqrt(new_accum)[..., None]
    return (new_rows, new_accum, dense_grad)


def solution(mesh):
    fine = Mesh(mesh.devices.reshape(4, 4, 2, 2, 2), every)
    samples = P(every)
    owned = P(("y", "x", "zh", "c"), "zl")
    return jax.shard_map(
        per_device,
        mesh=fine,
        in_specs=(samples, samples, samples, owned, owned, samples, samples),
        out_specs=(owned, owned, P()),
        check_vma=False,
    )
```

```python
import functools

import jax
import jax.numpy as jnp
from jax import lax
from jax.experimental import pallas as pl
from jax.experimental.pallas import tpu as pltpu
from jax.sharding import Mesh, PartitionSpec as P


learn_rate = 0.5
ring = 4
every = ("y", "x", "zh", "c", "zl")
deep = ("zh", "zl")
f32 = jnp.float32
bf16 = jnp.bfloat16


def sized(row):
    size = (128 + (row & 127)) << ((row >> 7) & 7)
    return jnp.where(row >= 1024, -size, size)


def coded(row):
    return sized(row).astype(f32).astype(bf16)


def slot_codes(lengths, looked):
    rows = jnp.transpose(looked, (1, 2, 0))
    count = jnp.transpose(lengths, (1, 0))
    slots = rows.shape[1]
    active = [count > j for j in range(slots)]
    row = [rows[:, j, :] for j in range(slots)]
    codes, weights = [], []
    for j in range(slots):
        first = active[j]
        for i in range(j):
            first = first & (row[i] != row[j])
        weight = jnp.ones_like(count)
        for i in range(j + 1, slots):
            weight = weight + (active[i] & (row[i] == row[j])).astype(jnp.int32)
        codes.append(jnp.where(first, coded(row[j]), jnp.zeros((), bf16)))
        weights.append(weight.astype(f32).astype(bf16))
    return jnp.stack(codes + weights, axis=1)


def pack_kernel(*refs):
    grad_ref, out_ref, swap_ref = refs[0], refs[-2], refs[-1]
    samples, tables, width = grad_ref.shape

    @pl.when(pl.program_id(0) == 0)
    def _():
        to = lax.broadcasted_iota(jnp.int32, swap_ref.shape, 0)
        of = lax.broadcasted_iota(jnp.int32, swap_ref.shape, 1)
        hit = ((to & 15) == (of >> 4)) & ((to >> 4) == (of & 15))
        swap_ref[...] = jnp.where(hit, 1.0, 0.0).astype(bf16)

    for first in range(0, samples, 16):
        block = grad_ref[first : first + 16].reshape(16 * tables, width)
        turned = jnp.dot(swap_ref[...], block, preferred_element_type=f32)
        out_ref[:, first : first + 16, :] = turned.astype(bf16).reshape(tables, 16, width)
    if len(refs) == 4:
        out_ref[:, samples : samples + 8, :] = refs[1][...]


def packed(grads, part, codes=()):
    samples, tables, width = grads.shape
    count = samples // parts
    height = count + 8 * len(codes)
    return pl.pallas_call(
        pack_kernel,
        grid=(tables // 16,),
        in_specs=[pl.BlockSpec((count, 16, width), lambda i: (part, i, 0))]
        + [pl.BlockSpec((16, 8, width), lambda i: (i, 0, 0))] * len(codes),
        out_specs=pl.BlockSpec((16, height, width), lambda i: (i, 0, 0)),
        out_shape=jax.ShapeDtypeStruct((tables, height, width), bf16),
        scratch_shapes=[pltpu.VMEM((256, 256), bf16)],
        cost_estimate=pl.CostEstimate(flops=2 * 256 * count * tables * width, bytes_accessed=4 << 20, transcendentals=0),
        name="pack",
    )(grads, *codes)


parts = 2
group = 8
stripe = 256


def sum_kernel(part, base_ref, info_ref, data_ref, *refs):
    out_ref, mine_ref = refs[-2], refs[-1]
    senders, samples, _ = data_ref.shape
    rows = out_ref.shape[0]

    @pl.when(pl.program_id(0) == 0)
    def _():
        out_ref[...] = refs[0][...] if len(refs) == 3 else jnp.zeros_like(out_ref)
        mine_ref[...] = sized(base_ref[0] + lax.broadcasted_iota(jnp.int32, mine_ref.shape, 0)).astype(f32)

    zero = jnp.zeros((), bf16)
    here = slice(part * samples, (part + 1) * samples)
    for first in range(0, senders, group):
        pairs = [
            jnp.concatenate([info_ref[k][:, here], info_ref[k + 1][:, here]], axis=1)
            for k in range(first, first + group, 2)
        ]
        values = jnp.concatenate([data_ref[k, 0:samples, :] for k in range(first, first + group)], axis=0)
        for top in range(0, rows, stripe):
            mine = mine_ref[top : top + stripe, :].astype(bf16)
            hots = []
            for info in pairs:
                hot = jnp.where(mine == info[3:4], info[7:8], zero)
                for j in (2, 1, 0):
                    hot = jnp.where(mine == info[j : j + 1], info[4 + j : 5 + j], hot)
                hots.append(hot)
            out_ref[top : top + stripe, :] += jnp.dot(
                jnp.concatenate(hots, axis=1), values, preferred_element_type=f32
            )


def summed(part, first, data, base, rows, before=()):
    senders, _, width = data.shape
    samples = width // parts
    step = 16
    return pl.pallas_call(
        functools.partial(sum_kernel, part),
        grid_spec=pltpu.PrefetchScalarGridSpec(
            num_scalar_prefetch=1,
            grid=(senders // step,),
            in_specs=[
                pl.BlockSpec((step, 8, width), lambda i, b: (i, samples // 8, 0)),
                pl.BlockSpec((step, samples, width), lambda i, b: (i, 0, 0)),
            ]
            + [pl.BlockSpec((rows, width), lambda i, b: (b[0] // rows, 0))] * len(before),
            out_specs=pl.BlockSpec((rows, width), lambda i, b: (0, 0)),
            scratch_shapes=[pltpu.VMEM((rows, width), f32)],
        ),
        out_shape=jax.ShapeDtypeStruct((rows, width), f32),
        cost_estimate=pl.CostEstimate(flops=2 * senders * samples * rows * width, bytes_accessed=3 << 20, transcendentals=0),
        name="sum_by_row",
    )(base, first, data, *before)


def to_next(value, axis, step):
    return lax.ppermute(value, axis, [(i, (i + step) % ring) for i in range(ring)])


def scattered(value, axis, here):
    arrived = [
        to_next(lax.dynamic_index_in_dim(value, (here + step) & 3, 0, keepdims=False), axis, step)
        for step in range(1, ring)
    ]
    own = lax.dynamic_index_in_dim(value, here, 0, keepdims=False)
    return own + arrived[0] + arrived[1] + arrived[2]


def place_kernel(at_ref, *refs):
    out_ref = refs[-1]
    here_y, here_x, here_z, here_c = (at_ref[k] for k in range(4))
    for number, piece in enumerate(refs[:-1]):
        core, stream, far = number // 8, number // 4 % 2, number % 4
        c = here_c if core == 0 else 1 - here_c
        for near in range(ring):
            dy, dx = (far, near) if stream == 0 else (near, far)
            y = (here_y + ring - dy) % ring
            x = (here_x + ring - dx) % ring
            left = pl.multiple_of((x % 2) * 512 + stream * 256, 256)
            for dz in range(ring):
                z = (here_z + ring - dz) % ring
                top = pl.multiple_of((x // 2) * 512 + c * 256 + y * 64 + z * 16, 16)
                out_ref[pl.ds(top, 16), pl.ds(left, 256)] = piece[near, dz]


def placed(at, pieces):
    return pl.pallas_call(
        place_kernel,
        in_specs=[pl.BlockSpec(memory_space=pltpu.SMEM)] + [pl.BlockSpec(memory_space=pltpu.VMEM)] * len(pieces),
        out_specs=pl.BlockSpec(memory_space=pltpu.VMEM),
        out_shape=jax.ShapeDtypeStruct((1024, 1024), f32),
        cost_estimate=pl.CostEstimate(flops=3 << 20, bytes_accessed=8 << 20, transcendentals=0),
        name="place",
    )(at, *pieces)


def gathered(value, axis):
    return [value] + [to_next(value, axis, step) for step in range(1, ring)]


def dense_sum(inputs, cotangents):
    y, x, c = (lax.axis_index(a) for a in ("y", "x", "c"))
    z = lax.axis_index(deep)

    def share(of):
        one = jnp.where((of & 2) == 0, inputs[:, :512], inputs[:, 512:])
        two = jnp.where((of & 1) == 0, cotangents[:, :512], cotangents[:, 512:])
        return jnp.concatenate([one, two], axis=1)

    parts = [share(x)] + [to_next(share((x + step) & 3), "x", step) for step in range(1, ring)]
    both = jnp.concatenate(parts, axis=0)
    local = lax.dot_general(both[:, :512], both[:, 512:], (((0,), (0,)), ((), ())), preferred_element_type=f32)
    halves = local.reshape(2, 256, 512)
    swap = [(0, 1), (1, 0)]
    other = lax.ppermute(lax.dynamic_index_in_dim(halves, 1 - c, 0, keepdims=False), "c", swap)
    total = lax.dynamic_index_in_dim(halves, c, 0, keepdims=False) + other
    total = scattered(total.reshape(ring, 64, 512), "y", y)
    total = scattered(total.reshape(ring, 16, 512), deep, z)
    total = jnp.stack(gathered(total, deep))
    left, right = (total[..., :256], total[..., 256:])
    left = gathered(jnp.stack(gathered(left, "x")), "y")
    right = gathered(jnp.stack(gathered(right, "y")), "x")
    mine = left + right
    theirs = [lax.ppermute(p, "c", swap) for p in mine]
    return placed(jnp.stack([y, x, z, c]).astype(jnp.int32), mine + theirs)


def per_device(
    pooled_grad, bag_lengths, bag_rows, table_rows, row_accum, dense_input, dense_cotangent
):
    tables, rows = row_accum.shape
    dense_grad = dense_sum(dense_input, dense_cotangent)
    codes = slot_codes(bag_lengths, bag_rows)

    def exchanged(value):
        return lax.all_to_all(value, every, split_axis=0, concat_axis=0, tiled=True)

    first = exchanged(packed(pooled_grad, 0, (codes,)))
    second = exchanged(packed(pooled_grad, 1))
    half = lax.axis_index("zl").astype(jnp.int32)
    early = summed(0, first, first, jnp.zeros((1,), jnp.int32), tables * rows)
    theirs = summed(1, first, second, ((1 - half) * rows)[None], rows, (early,))
    arrived = lax.ppermute(theirs, "zl", [(0, 1), (1, 0)])
    own = summed(1, first, second, (half * rows)[None], rows, (early,))
    row_grad = jnp.where(half == 0, jnp.stack([own, arrived]), jnp.stack([arrived, own]))
    new_accum = row_accum + jnp.mean(row_grad * row_grad, axis=-1)
    new_rows = table_rows - learn_rate * row_grad / jnp.sqrt(new_accum)[..., None]
    return (new_rows, new_accum, dense_grad)


def solution(mesh):
    fine = Mesh(mesh.devices.reshape(4, 4, 2, 2, 2), every)
    samples = P(every)
    owned = P(("y", "x", "zh", "c"), "zl")
    return jax.shard_map(
        per_device,
        mesh=fine,
        in_specs=(samples, samples, samples, owned, owned, samples, samples),
        out_specs=(owned, owned, P()),
        check_vma=False,
    )
```

```python
import functools

import jax
import jax.numpy as jnp
from jax import lax
from jax.experimental import pallas as pl
from jax.experimental.pallas import tpu as pltpu
from jax.sharding import Mesh, PartitionSpec as P


learn_rate = 0.5
ring = 4
every = ("y", "x", "zh", "c", "zl")
deep = ("zh", "zl")
f32 = jnp.float32
bf16 = jnp.bfloat16


def sized(row):
    size = (128 + (row & 127)) << ((row >> 7) & 7)
    return jnp.where(row >= 1024, -size, size)


def coded(row):
    return sized(row).astype(f32).astype(bf16)


def slot_codes(lengths, looked):
    rows = jnp.transpose(looked, (1, 2, 0))
    count = jnp.transpose(lengths, (1, 0))
    slots = rows.shape[1]
    active = [count > j for j in range(slots)]
    row = [rows[:, j, :] for j in range(slots)]
    codes, weights = [], []
    for j in range(slots):
        first = active[j]
        for i in range(j):
            first = first & (row[i] != row[j])
        weight = jnp.ones_like(count)
        for i in range(j + 1, slots):
            weight = weight + (active[i] & (row[i] == row[j])).astype(jnp.int32)
        codes.append(jnp.where(first, coded(row[j]), jnp.zeros((), bf16)))
        weights.append(weight.astype(f32).astype(bf16))
    return jnp.stack(codes + weights, axis=1)


def pack_kernel(*refs):
    grad_ref, out_ref, swap_ref = refs[0], refs[-2], refs[-1]
    samples, tables, width = grad_ref.shape

    @pl.when(pl.program_id(0) == 0)
    def _():
        to = lax.broadcasted_iota(jnp.int32, swap_ref.shape, 0)
        of = lax.broadcasted_iota(jnp.int32, swap_ref.shape, 1)
        hit = ((to & 15) == (of >> 4)) & ((to >> 4) == (of & 15))
        swap_ref[...] = jnp.where(hit, 1.0, 0.0).astype(bf16)

    for first in range(0, samples, 16):
        for top in range(0, tables, 16):
            block = grad_ref[first : first + 16, top : top + 16].reshape(256, width)
            turned = jnp.dot(swap_ref[...], block, preferred_element_type=f32)
            out_ref[top : top + 16, first : first + 16, :] = turned.astype(bf16).reshape(16, 16, width)
    if len(refs) == 4:
        out_ref[:, samples : samples + 8, :] = refs[1][...]


def packed(grads, part, codes=()):
    samples, tables, width = grads.shape
    count = samples // parts
    height = count + 8 * len(codes)
    return pl.pallas_call(
        pack_kernel,
        grid=(tables // 64,),
        in_specs=[pl.BlockSpec((count, 64, width), lambda i: (part, i, 0))]
        + [pl.BlockSpec((64, 8, width), lambda i: (i, 0, 0))] * len(codes),
        out_specs=pl.BlockSpec((64, height, width), lambda i: (i, 0, 0)),
        out_shape=jax.ShapeDtypeStruct((tables, height, width), bf16),
        scratch_shapes=[pltpu.VMEM((256, 256), bf16)],
        cost_estimate=pl.CostEstimate(flops=2 * 256 * count * tables * width, bytes_accessed=4 << 20, transcendentals=0),
        name="pack",
    )(grads, *codes)


parts = 2
group = 16
stripe = 512


def sum_kernel(part, base_ref, info_ref, data_ref, *refs):
    out_ref, mine_ref = refs[-2], refs[-1]
    senders, samples, _ = data_ref.shape
    rows = out_ref.shape[0]

    @pl.when(pl.program_id(0) == 0)
    def _():
        out_ref[...] = refs[0][...] if len(refs) == 3 else jnp.zeros_like(out_ref)
        mine_ref[...] = sized(base_ref[0] + lax.broadcasted_iota(jnp.int32, mine_ref.shape, 0)).astype(f32)

    zero = jnp.zeros((), bf16)
    here = slice(part * samples, (part + 1) * samples)
    for first in range(0, senders, group):
        pairs = [
            jnp.concatenate([info_ref[k][:, here], info_ref[k + 1][:, here]], axis=1)
            for k in range(first, first + group, 2)
        ]
        values = jnp.concatenate([data_ref[k, 0:samples, :] for k in range(first, first + group)], axis=0)
        for top in range(0, rows, stripe):
            mine = mine_ref[top : top + stripe, :].astype(bf16)
            hots = []
            for info in pairs:
                hot = jnp.where(mine == info[3:4], info[7:8], zero)
                for j in (2, 1, 0):
                    hot = jnp.where(mine == info[j : j + 1], info[4 + j : 5 + j], hot)
                hots.append(hot)
            out_ref[top : top + stripe, :] += jnp.dot(
                jnp.concatenate(hots, axis=1), values, preferred_element_type=f32
            )


def summed(part, first, data, base, rows, before=()):
    senders, _, width = data.shape
    samples = width // parts
    step = 32
    return pl.pallas_call(
        functools.partial(sum_kernel, part),
        grid_spec=pltpu.PrefetchScalarGridSpec(
            num_scalar_prefetch=1,
            grid=(senders // step,),
            in_specs=[
                pl.BlockSpec((step, 8, width), lambda i, b: (i, samples // 8, 0)),
                pl.BlockSpec((step, samples, width), lambda i, b: (i, 0, 0)),
            ]
            + [pl.BlockSpec((rows, width), lambda i, b: (b[0] // rows, 0))] * len(before),
            out_specs=pl.BlockSpec((rows, width), lambda i, b: (0, 0)),
            scratch_shapes=[pltpu.VMEM((rows, width), f32)],
        ),
        out_shape=jax.ShapeDtypeStruct((rows, width), f32),
        cost_estimate=pl.CostEstimate(flops=2 * senders * samples * rows * width, bytes_accessed=3 << 20, transcendentals=0),
        name="sum_by_row",
    )(base, first, data, *before)


def to_next(value, axis, step):
    return lax.ppermute(value, axis, [(i, (i + step) % ring) for i in range(ring)])


def scattered(value, axis, here):
    arrived = [
        to_next(lax.dynamic_index_in_dim(value, (here + step) & 3, 0, keepdims=False), axis, step)
        for step in range(1, ring)
    ]
    own = lax.dynamic_index_in_dim(value, here, 0, keepdims=False)
    return own + arrived[0] + arrived[1] + arrived[2]


def place_kernel(at_ref, *refs):
    out_ref = refs[-1]
    here_y, here_x, here_c = (at_ref[k] for k in range(3))
    for number, piece in enumerate(refs[:-1]):
        c = here_c if number < ring else 1 - here_c
        y = (here_y - number) & 3
        for dx in range(ring):
            x = (here_x - dx) & 3
            left = pl.multiple_of((x & 1) * 512, 512)
            top = pl.multiple_of((x >> 1) * 512 + c * 256 + y * 64, 64)
            out_ref[pl.ds(top, 64), pl.ds(left, 512)] = piece[dx]


def placed(at, pieces):
    return pl.pallas_call(
        place_kernel,
        in_specs=[pl.BlockSpec(memory_space=pltpu.SMEM)] + [pl.BlockSpec(memory_space=pltpu.VMEM)] * len(pieces),
        out_specs=pl.BlockSpec(memory_space=pltpu.VMEM),
        out_shape=jax.ShapeDtypeStruct((1024, 1024), f32),
        cost_estimate=pl.CostEstimate(flops=3 << 20, bytes_accessed=8 << 20, transcendentals=0),
        name="place",
    )(at, *pieces)


def gathered(value, axis):
    return [value] + [to_next(value, axis, step) for step in range(1, ring)]


def dense_sum(inputs, cotangents):
    y, x, c = (lax.axis_index(a) for a in ("y", "x", "c"))

    def share(of):
        one = jnp.where((of & 2) == 0, inputs[:, :512], inputs[:, 512:])
        two = jnp.where((of & 1) == 0, cotangents[:, :512], cotangents[:, 512:])
        return jnp.concatenate([one, two], axis=1)

    parts = [share(x)] + [to_next(share((x + step) & 3), "x", step) for step in range(1, ring)]
    both = jnp.concatenate(parts, axis=0)
    local = lax.dot_general(both[:, :512], both[:, 512:], (((0,), (0,)), ((), ())), preferred_element_type=f32)
    halves = local.reshape(2, 256, 512)
    swap = [(0, 1), (1, 0)]
    other = lax.ppermute(lax.dynamic_index_in_dim(halves, 1 - c, 0, keepdims=False), "c", swap)
    total = lax.dynamic_index_in_dim(halves, c, 0, keepdims=False) + other
    total = scattered(total.reshape(ring, 64, 512), "y", y)
    ranks = gathered(total, deep)
    total = (ranks[0] + ranks[2]) + (ranks[1] + ranks[3])
    mine = gathered(jnp.stack(gathered(total, "x")), "y")
    theirs = [lax.ppermute(p, "c", swap) for p in mine]
    return placed(jnp.stack([y, x, c]).astype(jnp.int32), mine + theirs)


def per_device(
    pooled_grad, bag_lengths, bag_rows, table_rows, row_accum, dense_input, dense_cotangent
):
    tables, rows = row_accum.shape
    dense_grad = dense_sum(dense_input, dense_cotangent)
    codes = slot_codes(bag_lengths, bag_rows)

    def exchanged(value):
        return lax.all_to_all(value, every, split_axis=0, concat_axis=0, tiled=True)

    near = packed(pooled_grad, 0, (codes,))
    late = packed(pooled_grad, 1)
    first = exchanged(near)
    second = exchanged(late)
    half = lax.axis_index("zl").astype(jnp.int32)
    early = summed(0, first, first, jnp.zeros((1,), jnp.int32), tables * rows)
    theirs = summed(1, first, second, ((1 - half) * rows)[None], rows, (early,))
    arrived = lax.ppermute(theirs, "zl", [(0, 1), (1, 0)])
    own = summed(1, first, second, (half * rows)[None], rows, (early,))
    row_grad = jnp.where(half == 0, jnp.stack([own, arrived]), jnp.stack([arrived, own]))
    new_accum = row_accum + jnp.mean(row_grad * row_grad, axis=-1)
    new_rows = table_rows - learn_rate * row_grad / jnp.sqrt(new_accum)[..., None]
    return (new_rows, new_accum, dense_grad)


def solution(mesh):
    fine = Mesh(mesh.devices.reshape(4, 4, 2, 2, 2), every)
    samples = P(every)
    owned = P(("y", "x", "zh", "c"), "zl")
    return jax.shard_map(
        per_device,
        mesh=fine,
        in_specs=(samples, samples, samples, owned, owned, samples, samples),
        out_specs=(owned, owned, P()),
        check_vma=False,
    )
```

```python
import functools

import jax
import jax.numpy as jnp
from jax import lax
from jax.experimental import pallas as pl
from jax.experimental.pallas import tpu as pltpu
from jax.sharding import Mesh, PartitionSpec as P


learn_rate = 0.5
ring = 4
every = ("y", "x", "zh", "c", "zl")
deep = ("zh", "zl")
f32 = jnp.float32
bf16 = jnp.bfloat16


def sized(row):
    size = (128 + (row & 127)) << ((row >> 7) & 7)
    return jnp.where(row >= 1024, -size, size)


def coded(row):
    return sized(row).astype(f32).astype(bf16)


def slot_codes(lengths, looked):
    rows = jnp.transpose(looked, (1, 2, 0))
    count = jnp.transpose(lengths, (1, 0))
    slots = rows.shape[1]
    active = [count > j for j in range(slots)]
    row = [rows[:, j, :] for j in range(slots)]
    codes, weights = [], []
    for j in range(slots):
        first = active[j]
        for i in range(j):
            first = first & (row[i] != row[j])
        weight = jnp.ones_like(count)
        for i in range(j + 1, slots):
            weight = weight + (active[i] & (row[i] == row[j])).astype(jnp.int32)
        codes.append(jnp.where(first, coded(row[j]), jnp.zeros((), bf16)))
        weights.append(weight.astype(f32).astype(bf16))
    return jnp.stack(codes + weights, axis=1)


def pack_kernel(*refs):
    grad_ref, out_ref, swap_ref = refs[0], refs[-2], refs[-1]
    samples, tables, width = grad_ref.shape

    @pl.when(pl.program_id(0) == 0)
    def _():
        to = lax.broadcasted_iota(jnp.int32, swap_ref.shape, 0)
        of = lax.broadcasted_iota(jnp.int32, swap_ref.shape, 1)
        hit = ((to & 15) == (of >> 4)) & ((to >> 4) == (of & 15))
        swap_ref[...] = jnp.where(hit, 1.0, 0.0).astype(bf16)

    for first in range(0, samples, 16):
        for top in range(0, tables, 16):
            block = grad_ref[first : first + 16, top : top + 16].reshape(256, width)
            turned = jnp.dot(swap_ref[...], block, preferred_element_type=f32)
            out_ref[top : top + 16, first : first + 16, :] = turned.astype(bf16).reshape(16, 16, width)
    if len(refs) == 4:
        out_ref[:, samples : samples + 8, :] = refs[1][...]


def packed(grads, part, codes=()):
    start, stop = cut[part : part + 2]
    _, tables, width = grads.shape
    count = stop - start
    height = count + 8 * len(codes)
    return pl.pallas_call(
        pack_kernel,
        grid=(tables // 64,),
        in_specs=[pl.BlockSpec((pl.Element(count), pl.Element(64), pl.Element(width)), lambda i: (start, i * 64, 0))]
        + [pl.BlockSpec((64, 8, width), lambda i: (i, 0, 0))] * len(codes),
        out_specs=pl.BlockSpec((64, height, width), lambda i: (i, 0, 0)),
        out_shape=jax.ShapeDtypeStruct((tables, height, width), bf16),
        scratch_shapes=[pltpu.VMEM((256, 256), bf16)],
        cost_estimate=pl.CostEstimate(flops=2 * 256 * count * tables * width, bytes_accessed=4 << 20, transcendentals=0),
        name="pack",
    )(grads, *codes)


cut = (0, 80, 128)
group = 16
stripe = 512


def sum_kernel(part, base_ref, info_ref, data_ref, *refs):
    out_ref, mine_ref = refs[-2], refs[-1]
    senders, samples, width = data_ref.shape
    rows = out_ref.shape[0]

    @pl.when(pl.program_id(0) == 0)
    def _():
        out_ref[...] = refs[0][...] if len(refs) == 3 else jnp.zeros_like(out_ref)
        mine_ref[...] = sized(base_ref[0] + lax.broadcasted_iota(jnp.int32, mine_ref.shape, 0)).astype(f32)

    zero = jnp.zeros((), bf16)
    here = slice(*cut[part : part + 2])
    for first in range(0, senders, group):
        infos = jnp.concatenate([info_ref[k][:, here] for k in range(first, first + group)], axis=1)
        infos = [infos[:, k : k + width] for k in range(0, group * samples, width)]
        values = jnp.concatenate([data_ref[k, 0:samples, :] for k in range(first, first + group)], axis=0)
        for top in range(0, rows, stripe):
            mine = mine_ref[top : top + stripe, :].astype(bf16)
            hots = []
            for info in infos:
                hot = jnp.where(mine == info[3:4], info[7:8], zero)
                for j in (2, 1, 0):
                    hot = jnp.where(mine == info[j : j + 1], info[4 + j : 5 + j], hot)
                hots.append(hot)
            out_ref[top : top + stripe, :] += jnp.dot(
                jnp.concatenate(hots, axis=1), values, preferred_element_type=f32
            )


def summed(part, first, data, base, rows, before=()):
    senders, _, width = data.shape
    samples = cut[part + 1] - cut[part]
    step = 32
    return pl.pallas_call(
        functools.partial(sum_kernel, part),
        grid_spec=pltpu.PrefetchScalarGridSpec(
            num_scalar_prefetch=1,
            grid=(senders // step,),
            in_specs=[
                pl.BlockSpec((step, 8, width), lambda i, b: (i, cut[1] // 8, 0)),
                pl.BlockSpec((step, samples, width), lambda i, b: (i, 0, 0)),
            ]
            + [pl.BlockSpec((rows, width), lambda i, b: (b[0] // rows, 0))] * len(before),
            out_specs=pl.BlockSpec((rows, width), lambda i, b: (0, 0)),
            scratch_shapes=[pltpu.VMEM((rows, width), f32)],
        ),
        out_shape=jax.ShapeDtypeStruct((rows, width), f32),
        cost_estimate=pl.CostEstimate(flops=2 * senders * samples * rows * width, bytes_accessed=3 << 20, transcendentals=0),
        name="sum_by_row",
    )(base, first, data, *before)


def to_next(value, axis, step):
    return lax.ppermute(value, axis, [(i, (i + step) % ring) for i in range(ring)])


def scattered(value, axis, here):
    arrived = [
        to_next(lax.dynamic_index_in_dim(value, (here + step) & 3, 0, keepdims=False), axis, step)
        for step in range(1, ring)
    ]
    own = lax.dynamic_index_in_dim(value, here, 0, keepdims=False)
    return own + arrived[0] + arrived[1] + arrived[2]


def step_of(power, factor):
    return jnp.exp2(power.astype(f32)) * (factor.astype(f32) * (1 / 32767 / 8192))


def code_kernel(*refs):
    out_ref = refs[-1]
    total = (refs[0][...] + refs[2][...]) + (refs[1][...] + refs[3][...])
    top = jnp.max(jnp.abs(total), axis=1, keepdims=True)
    power = jnp.clip(jnp.floor(jnp.log2(jnp.maximum(top, 1e-30))), -90.0, 90.0).astype(jnp.int32)
    factor = jnp.ceil(top * jnp.exp2(-power.astype(f32)) * 8192).astype(jnp.int32)
    factor = jnp.clip(factor, 0, 32767)
    step = step_of(power, factor)
    value = jnp.round(total * jnp.where(step > 0, 1 / step, 0.0))
    value = jnp.clip(value, -32767, 32767).astype(jnp.int32)
    lane = lax.broadcasted_iota(jnp.int32, (total.shape[0], 128), 1)
    out_ref[:, :512] = value.astype(jnp.int16)
    out_ref[:, 512:] = jnp.where(lane == 0, power, factor).astype(jnp.int16)


def coded_sum(ranks):
    return pl.pallas_call(
        code_kernel,
        out_shape=jax.ShapeDtypeStruct((64, 640), jnp.int16),
        cost_estimate=pl.CostEstimate(flops=1 << 20, bytes_accessed=1 << 20, transcendentals=0),
        name="code_sum",
    )(*ranks)


def place_kernel(at_ref, *refs):
    pieces, out_ref, held, sems = refs[: 2 * ring], refs[-3], refs[-2], refs[-1]
    here_y, here_x, here_c = (at_ref[k] for k in range(3))
    copies = []
    for number, piece in enumerate(pieces):
        c = here_c if number < ring else 1 - here_c
        y = (here_y - number) & 3
        for dx in range(ring):
            x = (here_x - dx) & 3
            left = pl.multiple_of((x & 1) * 512, 512)
            top = pl.multiple_of((x >> 1) * 512 + c * 256 + y * 64, 64)
            block = piece[dx].astype(jnp.int32)
            step = step_of(block[:, 512:513], block[:, 513:514])
            held[number, dx] = block[:, :512].astype(f32) * step
            copies.append(
                pltpu.make_async_copy(
                    held.at[number, dx], out_ref.at[pl.ds(top, 64), pl.ds(left, 512)], sems.at[number, dx]
                )
            )
            copies[-1].start()
    for copy in copies:
        copy.wait()


def placed(at, pieces):
    return pl.pallas_call(
        place_kernel,
        in_specs=[pl.BlockSpec(memory_space=pltpu.SMEM)] + [pl.BlockSpec(memory_space=pltpu.VMEM)] * len(pieces),
        out_specs=pl.BlockSpec(memory_space=pl.ANY),
        out_shape=jax.ShapeDtypeStruct((1024, 1024), f32),
        scratch_shapes=[
            pltpu.VMEM((2 * ring, ring, 64, 512), f32),
            pltpu.SemaphoreType.DMA((2 * ring, ring)),
        ],
        cost_estimate=pl.CostEstimate(flops=3 << 20, bytes_accessed=8 << 20, transcendentals=0),
        name="place",
    )(at, *pieces)


def share_kernel(at_ref, left_ref, right_ref, *out_refs):
    for step, out_ref in enumerate(out_refs):
        of = (at_ref[0] + step) & 3
        out_ref[:, :512] = left_ref[:, pl.ds(pl.multiple_of((of >> 1) * 512, 512), 512)]
        out_ref[:, 512:] = right_ref[:, pl.ds(pl.multiple_of((of & 1) * 512, 512), 512)]


def shares(x, inputs, cotangents):
    return pl.pallas_call(
        share_kernel,
        in_specs=[pl.BlockSpec(memory_space=pltpu.SMEM)] + [pl.BlockSpec(memory_space=pltpu.VMEM)] * 2,
        out_shape=[jax.ShapeDtypeStruct(inputs.shape, bf16)] * ring,
        cost_estimate=pl.CostEstimate(flops=1 << 19, bytes_accessed=2 << 20, transcendentals=0),
        name="share",
    )(x[None], inputs, cotangents)


def gathered(value, axis):
    return [value] + [to_next(value, axis, step) for step in range(1, ring)]


def dense_sum(inputs, cotangents):
    y, x, c = (lax.axis_index(a) for a in ("y", "x", "c"))

    parts = shares(x.astype(jnp.int32), inputs, cotangents)
    parts = [parts[0]] + [to_next(parts[step], "x", step) for step in range(1, ring)]
    both = jnp.concatenate(parts, axis=0)
    local = lax.dot_general(both[:, :512], both[:, 512:], (((0,), (0,)), ((), ())), preferred_element_type=f32)
    halves = local.reshape(2, 256, 512)
    swap = [(0, 1), (1, 0)]
    other = lax.ppermute(lax.dynamic_index_in_dim(halves, 1 - c, 0, keepdims=False), "c", swap)
    total = lax.dynamic_index_in_dim(halves, c, 0, keepdims=False) + other
    total = scattered(total.reshape(ring, 64, 512), "y", y)
    ranks = gathered(total, deep)
    total = coded_sum(ranks)
    mine = gathered(jnp.stack(gathered(total, "x")), "y")
    theirs = [lax.ppermute(p, "c", swap) for p in mine]
    return placed(jnp.stack([y, x, c]).astype(jnp.int32), mine + theirs)


def update_kernel(at_ref, table_ref, accum_ref, prior_ref, grad_ref, *refs):
    out_ref, new_ref = refs[-2:]
    at = at_ref[0]
    accum = jnp.where(at == 0, accum_ref[0:1, :], accum_ref[1:2, :])
    for top in range(0, grad_ref.shape[0], 128):
        span = slice(top, top + 128)
        grad = grad_ref[span, :]
        before = jnp.broadcast_to(accum[:, span], (128, 128)).T
        after = before + jnp.mean(grad * grad, axis=1, keepdims=True)
        out_ref[0, span, :] = table_ref[0, span, :] - learn_rate * grad / jnp.sqrt(after)
        row = after.T[0:1, :]
        new_ref[0:1, span] = jnp.where(at == 0, row, prior_ref[0:1, span])
        new_ref[1:2, span] = jnp.where(at == 0, prior_ref[1:2, span], row)


def updated(at, table_rows, row_accum, prior, grad, before=()):
    tables, rows, width = table_rows.shape
    small = pl.BlockSpec((tables, rows), lambda i, b: (0, 0))
    return pl.pallas_call(
        update_kernel,
        grid_spec=pltpu.PrefetchScalarGridSpec(
            num_scalar_prefetch=1,
            grid=(1,),
            in_specs=[
                pl.BlockSpec((1, rows, width), lambda i, b: (b[0], 0, 0)),
                small,
                small,
                pl.BlockSpec((rows, width), lambda i, b: (0, 0)),
            ]
            + [pl.BlockSpec(memory_space=pl.ANY)] * len(before),
            out_specs=[pl.BlockSpec((1, rows, width), lambda i, b: (b[0], 0, 0)), small],
        ),
        out_shape=[jax.ShapeDtypeStruct(table_rows.shape, f32), jax.ShapeDtypeStruct(row_accum.shape, f32)],
        input_output_aliases={5: 0} if before else {},
        cost_estimate=pl.CostEstimate(flops=1 << 20, bytes_accessed=2 << 20, transcendentals=0),
        name="update",
    )(at[None], table_rows, row_accum, prior, grad, *before)


def per_device(
    pooled_grad, bag_lengths, bag_rows, table_rows, row_accum, dense_input, dense_cotangent
):
    tables, rows = row_accum.shape
    dense_grad = dense_sum(dense_input, dense_cotangent)
    codes = slot_codes(bag_lengths, bag_rows)

    def exchanged(value):
        return lax.all_to_all(value, every, split_axis=0, concat_axis=0, tiled=True)

    near = packed(pooled_grad, 0, (codes,))
    late = packed(pooled_grad, 1)
    first = exchanged(near)
    second = exchanged(late)
    half = lax.axis_index("zl").astype(jnp.int32)
    early = summed(0, first, first, jnp.zeros((1,), jnp.int32), tables * rows)
    theirs = summed(1, first, second, ((1 - half) * rows)[None], rows, (early,))
    arrived = lax.ppermute(theirs, "zl", [(0, 1), (1, 0)])
    own = summed(1, first, second, (half * rows)[None], rows, (early,))
    part_rows, part_accum = updated(half, table_rows, row_accum, row_accum, own)
    new_rows, new_accum = updated(1 - half, table_rows, row_accum, part_accum, arrived, (part_rows,))
    return (new_rows, new_accum, dense_grad)


def solution(mesh):
    fine = Mesh(mesh.devices.reshape(4, 4, 2, 2, 2), every)
    samples = P(every)
    owned = P(("y", "x", "zh", "c"), "zl")
    return jax.shard_map(
        per_device,
        mesh=fine,
        in_specs=(samples, samples, samples, owned, owned, samples, samples),
        out_specs=(owned, owned, P()),
        check_vma=False,
    )
```

```python
import functools

import jax
import jax.numpy as jnp
from jax import lax
from jax.experimental import pallas as pl
from jax.experimental.pallas import tpu as pltpu
from jax.sharding import Mesh, PartitionSpec as P


learn_rate = 0.5
ring = 4
every = ("y", "x", "zh", "c", "zl")
deep = ("zh", "zl")
f32 = jnp.float32
bf16 = jnp.bfloat16


def sized(row):
    size = (128 + (row & 127)) << ((row >> 7) & 7)
    return jnp.where(row >= 1024, -size, size)


def codes_kernel(row_ref, count_ref, out_ref):
    samples, slots, tables = row_ref.shape
    row = [row_ref[:, j, :] for j in range(slots)]
    active = [count_ref[...] > j for j in range(slots)]
    kinds = []
    for j in range(slots):
        first = active[j]
        for i in range(j):
            first = first & (row[i] != row[j])
        kinds.append(jnp.where(first, sized(row[j]), 0))
    for j in range(slots):
        weight = jnp.ones_like(row[j])
        for i in range(j + 1, slots):
            weight = weight + jnp.where(active[i] & (row[i] == row[j]), 1, 0)
        kinds.append(weight)
    kinds = [kind.astype(f32).T.astype(bf16) for kind in kinds]
    size = 16 * len(kinds)
    to = lax.broadcasted_iota(jnp.int32, (size, size), 0)
    of = lax.broadcasted_iota(jnp.int32, (size, size), 1)
    turn = jnp.where(((to & 7) == (of >> 4)) & ((to >> 3) == (of & 15)), 1.0, 0.0).astype(bf16)
    for top in range(0, tables, 16):
        block = jnp.concatenate([kind[top : top + 16, :] for kind in kinds], axis=0)
        turned = jnp.dot(turn, block, preferred_element_type=f32)
        out_ref[top : top + 16] = turned.reshape(16, len(kinds), samples).astype(bf16)


def slot_codes(lengths, looked):
    samples, tables, slots = looked.shape
    return pl.pallas_call(
        codes_kernel,
        out_shape=jax.ShapeDtypeStruct((tables, 2 * slots, samples), bf16),
        cost_estimate=pl.CostEstimate(flops=1 << 20, bytes_accessed=1 << 20, transcendentals=0),
        name="slot_codes",
    )(jnp.transpose(looked, (0, 2, 1)), lengths)


def pack_kernel(*refs):
    grad_ref, out_ref, swap_ref = refs[0], refs[-2], refs[-1]
    samples, tables, width = grad_ref.shape

    @pl.when(pl.program_id(0) == 0)
    def _():
        to = lax.broadcasted_iota(jnp.int32, swap_ref.shape, 0)
        of = lax.broadcasted_iota(jnp.int32, swap_ref.shape, 1)
        hit = ((to & 15) == (of >> 4)) & ((to >> 4) == (of & 15))
        swap_ref[...] = jnp.where(hit, 1.0, 0.0).astype(bf16)

    for first in range(0, samples, 16):
        for top in range(0, tables, 16):
            block = grad_ref[first : first + 16, top : top + 16].reshape(256, width)
            turned = jnp.dot(swap_ref[...], block, preferred_element_type=f32)
            out_ref[top : top + 16, first : first + 16, :] = turned.astype(bf16).reshape(16, 16, width)
    if len(refs) == 4:
        out_ref[:, samples : samples + 8, :] = refs[1][...]


def packed(grads, part, codes=()):
    start, stop = cut[part : part + 2]
    _, tables, width = grads.shape
    count = stop - start
    height = count + 8 * len(codes)
    return pl.pallas_call(
        pack_kernel,
        grid=(tables // 64,),
        in_specs=[pl.BlockSpec((pl.Element(count), pl.Element(64), pl.Element(width)), lambda i: (start, i * 64, 0))]
        + [pl.BlockSpec((64, 8, width), lambda i: (i, 0, 0))] * len(codes),
        out_specs=pl.BlockSpec((64, height, width), lambda i: (i, 0, 0)),
        out_shape=jax.ShapeDtypeStruct((tables, height, width), bf16),
        scratch_shapes=[pltpu.VMEM((256, 256), bf16)],
        cost_estimate=pl.CostEstimate(flops=2 * 256 * count * tables * width, bytes_accessed=4 << 20, transcendentals=0),
        name="pack",
    )(grads, *codes)


cut = (0, 80, 128)
group = 32
stripe = 512


def sum_kernel(part, base_ref, info_ref, data_ref, *refs):
    out_ref, mine_ref = refs[-2], refs[-1]
    senders, samples, width = data_ref.shape
    rows = out_ref.shape[0]

    @pl.when(pl.program_id(0) == 0)
    def _():
        out_ref[...] = refs[0][...] if len(refs) == 3 else jnp.zeros_like(out_ref)
        mine_ref[...] = sized(base_ref[0] + lax.broadcasted_iota(jnp.int32, mine_ref.shape, 0)).astype(f32)

    zero = jnp.zeros((), bf16)
    here = slice(*cut[part : part + 2])
    for first in range(0, senders, group):
        infos = jnp.concatenate([info_ref[k][:, here] for k in range(first, first + group)], axis=1)
        infos = [infos[:, k : k + width] for k in range(0, group * samples, width)]
        values = jnp.concatenate([data_ref[k, 0:samples, :] for k in range(first, first + group)], axis=0)
        for top in range(0, rows, stripe):
            mine = mine_ref[top : top + stripe, :].astype(bf16)
            hots = []
            for info in infos:
                hot = jnp.where(mine == info[3:4], info[7:8], zero)
                for j in (2, 1, 0):
                    hot = jnp.where(mine == info[j : j + 1], info[4 + j : 5 + j], hot)
                hots.append(hot)
            out_ref[top : top + stripe, :] += jnp.dot(
                jnp.concatenate(hots, axis=1), values, preferred_element_type=f32
            )


def summed(part, first, data, base, rows, before=()):
    senders, _, width = data.shape
    samples = cut[part + 1] - cut[part]
    step = 64
    return pl.pallas_call(
        functools.partial(sum_kernel, part),
        grid_spec=pltpu.PrefetchScalarGridSpec(
            num_scalar_prefetch=1,
            grid=(senders // step,),
            in_specs=[
                pl.BlockSpec((step, 8, width), lambda i, b: (i, cut[1] // 8, 0)),
                pl.BlockSpec((step, samples, width), lambda i, b: (i, 0, 0)),
            ]
            + [pl.BlockSpec((rows, width), lambda i, b: (b[0] // rows, 0))] * len(before),
            out_specs=pl.BlockSpec((rows, width), lambda i, b: (0, 0)),
            scratch_shapes=[pltpu.VMEM((rows, width), f32)],
        ),
        out_shape=jax.ShapeDtypeStruct((rows, width), f32),
        cost_estimate=pl.CostEstimate(flops=2 * senders * samples * rows * width, bytes_accessed=3 << 20, transcendentals=0),
        name="sum_by_row",
    )(base, first, data, *before)


def to_next(value, axis, step):
    return lax.ppermute(value, axis, [(i, (i + step) % ring) for i in range(ring)])


def scattered(value, axis, here):
    arrived = [
        to_next(lax.dynamic_index_in_dim(value, (here + step) & 3, 0, keepdims=False), axis, step)
        for step in range(1, ring)
    ]
    own = lax.dynamic_index_in_dim(value, here, 0, keepdims=False)
    return own + arrived[0] + arrived[1] + arrived[2]


def step_of(power, factor):
    return jnp.exp2(power.astype(f32)) * (factor.astype(f32) * (1 / 32767 / 8192))


def code_kernel(*refs):
    out_ref = refs[-1]
    total = (refs[0][...] + refs[2][...]) + (refs[1][...] + refs[3][...])
    top = jnp.max(jnp.abs(total), axis=1, keepdims=True)
    power = jnp.clip(jnp.floor(jnp.log2(jnp.maximum(top, 1e-30))), -90.0, 90.0).astype(jnp.int32)
    factor = jnp.ceil(top * jnp.exp2(-power.astype(f32)) * 8192).astype(jnp.int32)
    factor = jnp.clip(factor, 0, 32767)
    step = step_of(power, factor)
    value = jnp.round(total * jnp.where(step > 0, 1 / step, 0.0))
    value = jnp.clip(value, -32767, 32767).astype(jnp.int32)
    lane = lax.broadcasted_iota(jnp.int32, (total.shape[0], 128), 1)
    out_ref[:, :512] = value.astype(jnp.int16)
    out_ref[:, 512:] = jnp.where(lane == 0, power, factor).astype(jnp.int16)


def coded_sum(ranks):
    return pl.pallas_call(
        code_kernel,
        out_shape=jax.ShapeDtypeStruct((64, 640), jnp.int16),
        cost_estimate=pl.CostEstimate(flops=1 << 20, bytes_accessed=1 << 20, transcendentals=0),
        name="code_sum",
    )(*ranks)


def place_kernel(at_ref, *refs):
    pieces, (out_ref, held, sems, taken, ins) = refs[:2], refs[2:]
    here_x, here_c = at_ref[0], at_ref[1]
    loads = {}
    for core in range(2):
        for y in range(ring):
            load = pltpu.make_async_copy(pieces[core].at[y], taken.at[core, y], ins.at[core, y])
            load.start()
            loads[core, y] = load
    stores = []
    for core in range(2):
        c = here_c if core == 0 else 1 - here_c
        for y in range(ring):
            loads[core, y].wait()
            for dx in range(ring):
                x = (here_x - dx) & 3
                left = pl.multiple_of((x & 1) * 512, 512)
                top = pl.multiple_of((x >> 1) * 512 + c * 256 + y * 64, 64)
                block = taken[core, y, dx].astype(jnp.int32)
                step = step_of(block[:, 512:513], block[:, 513:514])
                held[core, y, dx] = block[:, :512].astype(f32) * step
                store = pltpu.make_async_copy(
                    held.at[core, y, dx], out_ref.at[pl.ds(top, 64), pl.ds(left, 512)], sems.at[core, y, dx]
                )
                store.start()
                stores.append(store)
    for store in stores:
        store.wait()


def placed(at, pieces):
    return pl.pallas_call(
        place_kernel,
        in_specs=[pl.BlockSpec(memory_space=pltpu.SMEM)] + [pl.BlockSpec(memory_space=pl.ANY)] * 2,
        out_specs=pl.BlockSpec(memory_space=pl.ANY),
        out_shape=jax.ShapeDtypeStruct((1024, 1024), f32),
        scratch_shapes=[
            pltpu.VMEM((2, ring, ring, 64, 512), f32),
            pltpu.SemaphoreType.DMA((2, ring, ring)),
            pltpu.VMEM((2, ring, ring, 64, 640), jnp.int16),
            pltpu.SemaphoreType.DMA((2, ring)),
        ],
        cost_estimate=pl.CostEstimate(flops=3 << 20, bytes_accessed=8 << 20, transcendentals=0),
        name="place",
    )(at, *pieces)


def share_kernel(at_ref, left_ref, right_ref, *out_refs):
    for step, out_ref in enumerate(out_refs):
        of = (at_ref[0] + step) & 3
        out_ref[:, :512] = left_ref[:, pl.ds(pl.multiple_of((of >> 1) * 512, 512), 512)]
        out_ref[:, 512:] = right_ref[:, pl.ds(pl.multiple_of((of & 1) * 512, 512), 512)]


def shares(x, inputs, cotangents):
    return pl.pallas_call(
        share_kernel,
        in_specs=[pl.BlockSpec(memory_space=pltpu.SMEM)] + [pl.BlockSpec(memory_space=pltpu.VMEM)] * 2,
        out_shape=[jax.ShapeDtypeStruct(inputs.shape, bf16)] * ring,
        cost_estimate=pl.CostEstimate(flops=1 << 19, bytes_accessed=2 << 20, transcendentals=0),
        name="share",
    )(x[None], inputs, cotangents)


def gathered(value, axis):
    return [value] + [to_next(value, axis, step) for step in range(1, ring)]


def dense_sum(inputs, cotangents):
    y, x, c = (lax.axis_index(a) for a in ("y", "x", "c"))

    parts = shares(x.astype(jnp.int32), inputs, cotangents)
    parts = [parts[0]] + [to_next(parts[step], "x", step) for step in range(1, ring)]
    both = jnp.concatenate(parts, axis=0)
    local = lax.dot_general(both[:, :512], both[:, 512:], (((0,), (0,)), ((), ())), preferred_element_type=f32)
    halves = local.reshape(2, 256, 512)
    swap = [(0, 1), (1, 0)]
    other = lax.ppermute(lax.dynamic_index_in_dim(halves, 1 - c, 0, keepdims=False), "c", swap)
    total = lax.dynamic_index_in_dim(halves, c, 0, keepdims=False) + other
    total = scattered(total.reshape(ring, 64, 512), "y", y)
    ranks = gathered(total, deep)
    total = coded_sum(ranks)
    total = jnp.stack(gathered(total, "x"))
    total = jnp.broadcast_to(total[None], (ring, *total.shape))
    mine = lax.all_to_all(total, "y", split_axis=0, concat_axis=0, tiled=True)
    theirs = lax.ppermute(mine, "c", swap)
    return placed(jnp.stack([x, c]).astype(jnp.int32), (mine, theirs))


def update_kernel(at_ref, table_ref, accum_ref, prior_ref, grad_ref, *refs):
    out_ref, new_ref = refs[-2:]
    at = at_ref[0]
    accum = jnp.where(at == 0, accum_ref[0:1, :], accum_ref[1:2, :])
    for top in range(0, grad_ref.shape[0], 128):
        span = slice(top, top + 128)
        grad = grad_ref[span, :]
        before = jnp.broadcast_to(accum[:, span], (128, 128)).T
        after = before + jnp.mean(grad * grad, axis=1, keepdims=True)
        out_ref[0, span, :] = table_ref[0, span, :] - learn_rate * grad / jnp.sqrt(after)
        row = after.T[0:1, :]
        new_ref[0:1, span] = jnp.where(at == 0, row, prior_ref[0:1, span])
        new_ref[1:2, span] = jnp.where(at == 0, prior_ref[1:2, span], row)


def updated(at, table_rows, row_accum, prior, grad, before=()):
    tables, rows, width = table_rows.shape
    small = pl.BlockSpec((tables, rows), lambda i, b: (0, 0))
    return pl.pallas_call(
        update_kernel,
        grid_spec=pltpu.PrefetchScalarGridSpec(
            num_scalar_prefetch=1,
            grid=(1,),
            in_specs=[
                pl.BlockSpec((1, rows, width), lambda i, b: (b[0], 0, 0)),
                small,
                small,
                pl.BlockSpec((rows, width), lambda i, b: (0, 0)),
            ]
            + [pl.BlockSpec(memory_space=pl.ANY)] * len(before),
            out_specs=[pl.BlockSpec((1, rows, width), lambda i, b: (b[0], 0, 0)), small],
        ),
        out_shape=[jax.ShapeDtypeStruct(table_rows.shape, f32), jax.ShapeDtypeStruct(row_accum.shape, f32)],
        input_output_aliases={5: 0} if before else {},
        cost_estimate=pl.CostEstimate(flops=1 << 20, bytes_accessed=2 << 20, transcendentals=0),
        name="update",
    )(at[None], table_rows, row_accum, prior, grad, *before)


def per_device(
    pooled_grad, bag_lengths, bag_rows, table_rows, row_accum, dense_input, dense_cotangent
):
    tables, rows = row_accum.shape
    dense_grad = dense_sum(dense_input, dense_cotangent)
    codes = slot_codes(bag_lengths, bag_rows)

    def exchanged(value):
        return lax.all_to_all(value, every, split_axis=0, concat_axis=0, tiled=True)

    near = packed(pooled_grad, 0, (codes,))
    late = packed(pooled_grad, 1)
    first = exchanged(near)
    second = exchanged(late)
    half = lax.axis_index("zl").astype(jnp.int32)
    early = summed(0, first, first, jnp.zeros((1,), jnp.int32), tables * rows)
    theirs = summed(1, first, second, ((1 - half) * rows)[None], rows, (early,))
    arrived = lax.ppermute(theirs, "zl", [(0, 1), (1, 0)])
    own = summed(1, first, second, (half * rows)[None], rows, (early,))
    part_rows, part_accum = updated(half, table_rows, row_accum, row_accum, own)
    new_rows, new_accum = updated(1 - half, table_rows, row_accum, part_accum, arrived, (part_rows,))
    return (new_rows, new_accum, dense_grad)


def solution(mesh):
    fine = Mesh(mesh.devices.reshape(4, 4, 2, 2, 2), every)
    samples = P(every)
    owned = P(("y", "x", "zh", "c"), "zl")
    return jax.shard_map(
        per_device,
        mesh=fine,
        in_specs=(samples, samples, samples, owned, owned, samples, samples),
        out_specs=(owned, owned, P()),
        check_vma=False,
    )
```

```python
import functools

import jax
import jax.numpy as jnp
from jax import lax
from jax.experimental import pallas as pl
from jax.experimental.pallas import tpu as pltpu
from jax.sharding import Mesh, PartitionSpec as P


learn_rate = 0.5
ring = 4
every = ("y", "x", "zh", "c", "zl")
deep = ("zh", "zl")
f32 = jnp.float32
bf16 = jnp.bfloat16


def sized(row):
    size = (128 + (row & 127)) << ((row >> 7) & 7)
    return jnp.where(row >= 1024, -size, size)


def codes_kernel(row_ref, count_ref, out_ref):
    samples, slots, tables = row_ref.shape
    row = [row_ref[:, j, :] for j in range(slots)]
    active = [count_ref[...] > j for j in range(slots)]
    kinds = []
    for j in range(slots):
        first = active[j]
        for i in range(j):
            first = first & (row[i] != row[j])
        kinds.append(jnp.where(first, sized(row[j]), 0))
    for j in range(slots):
        weight = jnp.ones_like(row[j])
        for i in range(j + 1, slots):
            weight = weight + jnp.where(active[i] & (row[i] == row[j]), 1, 0)
        kinds.append(weight)
    kinds = [kind.astype(f32).T.astype(bf16) for kind in kinds]
    size = 16 * len(kinds)
    to = lax.broadcasted_iota(jnp.int32, (size, size), 0)
    of = lax.broadcasted_iota(jnp.int32, (size, size), 1)
    turn = jnp.where(((to & 7) == (of >> 4)) & ((to >> 3) == (of & 15)), 1.0, 0.0).astype(bf16)
    for top in range(0, tables, 16):
        block = jnp.concatenate([kind[top : top + 16, :] for kind in kinds], axis=0)
        turned = jnp.dot(turn, block, preferred_element_type=f32)
        out_ref[top : top + 16] = turned.reshape(16, len(kinds), samples).astype(bf16)


def slot_codes(lengths, looked):
    samples, tables, slots = looked.shape
    return pl.pallas_call(
        codes_kernel,
        out_shape=jax.ShapeDtypeStruct((tables, 2 * slots, samples), bf16),
        cost_estimate=pl.CostEstimate(flops=1 << 20, bytes_accessed=1 << 20, transcendentals=0),
        name="slot_codes",
    )(jnp.transpose(looked, (0, 2, 1)), lengths)


def pack_kernel(*refs):
    grad_ref, out_ref, swap_ref = refs[0], refs[-2], refs[-1]
    samples, tables, width = grad_ref.shape

    @pl.when(pl.program_id(0) == 0)
    def _():
        to = lax.broadcasted_iota(jnp.int32, swap_ref.shape, 0)
        of = lax.broadcasted_iota(jnp.int32, swap_ref.shape, 1)
        hit = ((to & 15) == (of >> 4)) & ((to >> 4) == (of & 15))
        swap_ref[...] = jnp.where(hit, 1.0, 0.0).astype(bf16)

    for first in range(0, samples, 16):
        for top in range(0, tables, 16):
            block = grad_ref[first : first + 16, top : top + 16].reshape(256, width)
            turned = jnp.dot(swap_ref[...], block, preferred_element_type=f32)
            out_ref[top : top + 16, first : first + 16, :] = turned.astype(bf16).reshape(16, 16, width)
    if len(refs) == 4:
        out_ref[:, samples : samples + 8, :] = refs[1][...]


def packed(grads, part, codes=()):
    start, stop = cut[part : part + 2]
    _, tables, width = grads.shape
    count = stop - start
    height = count + 8 * len(codes)
    return pl.pallas_call(
        pack_kernel,
        grid=(tables // 64,),
        in_specs=[pl.BlockSpec((pl.Element(count), pl.Element(64), pl.Element(width)), lambda i: (start, i * 64, 0))]
        + [pl.BlockSpec((64, 8, width), lambda i: (i, 0, 0))] * len(codes),
        out_specs=pl.BlockSpec((64, height, width), lambda i: (i, 0, 0)),
        out_shape=jax.ShapeDtypeStruct((tables, height, width), bf16),
        scratch_shapes=[pltpu.VMEM((256, 256), bf16)],
        cost_estimate=pl.CostEstimate(flops=2 * 256 * count * tables * width, bytes_accessed=4 << 20, transcendentals=0),
        name="pack",
    )(grads, *codes)


cut = (0, 80, 128)
group = 32
stripe = 512


def sum_kernel(part, base_ref, info_ref, data_ref, *refs):
    out_ref, mine_ref = refs[-2], refs[-1]
    senders, samples, width = data_ref.shape
    rows = out_ref.shape[0]

    @pl.when(pl.program_id(0) == 0)
    def _():
        out_ref[...] = refs[0][...] if len(refs) == 3 else jnp.zeros_like(out_ref)
        mine_ref[...] = sized(base_ref[0] + lax.broadcasted_iota(jnp.int32, mine_ref.shape, 0)).astype(f32)

    zero = jnp.zeros((), bf16)
    here = slice(*cut[part : part + 2])
    for first in range(0, senders, group):
        infos = jnp.concatenate([info_ref[k][:, here] for k in range(first, first + group)], axis=1)
        infos = [infos[:, k : k + width] for k in range(0, group * samples, width)]
        values = jnp.concatenate([data_ref[k, 0:samples, :] for k in range(first, first + group)], axis=0)
        for top in range(0, rows, stripe):
            mine = mine_ref[top : top + stripe, :].astype(bf16)
            hots = []
            for info in infos:
                hot = jnp.where(mine == info[3:4], info[7:8], zero)
                for j in (2, 1, 0):
                    hot = jnp.where(mine == info[j : j + 1], info[4 + j : 5 + j], hot)
                hots.append(hot)
            out_ref[top : top + stripe, :] += jnp.dot(
                jnp.concatenate(hots, axis=1), values, preferred_element_type=f32
            )


def summed(part, first, data, base, rows, before=()):
    senders, _, width = data.shape
    samples = cut[part + 1] - cut[part]
    step = 64
    return pl.pallas_call(
        functools.partial(sum_kernel, part),
        grid_spec=pltpu.PrefetchScalarGridSpec(
            num_scalar_prefetch=1,
            grid=(senders // step,),
            in_specs=[
                pl.BlockSpec((step, 8, width), lambda i, b: (i, cut[1] // 8, 0)),
                pl.BlockSpec((step, samples, width), lambda i, b: (i, 0, 0)),
            ]
            + [pl.BlockSpec((rows, width), lambda i, b: (b[0] // rows, 0))] * len(before),
            out_specs=pl.BlockSpec((rows, width), lambda i, b: (0, 0)),
            scratch_shapes=[pltpu.VMEM((rows, width), f32)],
        ),
        out_shape=jax.ShapeDtypeStruct((rows, width), f32),
        cost_estimate=pl.CostEstimate(flops=2 * senders * samples * rows * width, bytes_accessed=3 << 20, transcendentals=0),
        name="sum_by_row",
    )(base, first, data, *before)


def to_next(value, axis, step):
    return lax.ppermute(value, axis, [(i, (i + step) % ring) for i in range(ring)])


def scattered(value, axis, here):
    arrived = [
        to_next(lax.dynamic_index_in_dim(value, (here + step) & 3, 0, keepdims=False), axis, step)
        for step in range(1, ring)
    ]
    own = lax.dynamic_index_in_dim(value, here, 0, keepdims=False)
    return own + arrived[0] + arrived[1] + arrived[2]


def step_of(power, factor):
    return jnp.exp2(power.astype(f32)) * (factor.astype(f32) * (1 / 32767 / 8192))


def code_kernel(*refs):
    out_ref = refs[-1]
    total = (refs[0][...] + refs[2][...]) + (refs[1][...] + refs[3][...])
    top = jnp.max(jnp.abs(total), axis=1, keepdims=True)
    power = jnp.clip(jnp.floor(jnp.log2(jnp.maximum(top, 1e-30))), -90.0, 90.0).astype(jnp.int32)
    factor = jnp.ceil(top * jnp.exp2(-power.astype(f32)) * 8192).astype(jnp.int32)
    factor = jnp.clip(factor, 0, 32767)
    step = step_of(power, factor)
    value = jnp.round(total * jnp.where(step > 0, 1 / step, 0.0))
    value = jnp.clip(value, -32767, 32767).astype(jnp.int32)
    lane = lax.broadcasted_iota(jnp.int32, (total.shape[0], 128), 1)
    out_ref[:, :512] = value.astype(jnp.int16)
    out_ref[:, 512:] = jnp.where(lane == 0, power, factor).astype(jnp.int16)


def coded_sum(ranks):
    return pl.pallas_call(
        code_kernel,
        out_shape=jax.ShapeDtypeStruct((64, 640), jnp.int16),
        cost_estimate=pl.CostEstimate(flops=1 << 20, bytes_accessed=1 << 20, transcendentals=0),
        compiler_params=pltpu.CompilerParams(vmem_limit_bytes=4 << 20),
        name="code_sum",
    )(*ranks)


def place_kernel(at_ref, *refs):
    pieces, out_ref, held, sems = refs[: 2 * ring], refs[-3], refs[-2], refs[-1]
    here_y, here_x, here_c = (at_ref[k] for k in range(3))
    copies = []
    for number, piece in enumerate(pieces):
        c = here_c if number < ring else 1 - here_c
        y = (here_y - number) & 3
        for dx in range(ring):
            x = (here_x - dx) & 3
            left = pl.multiple_of((x & 1) * 512, 512)
            top = pl.multiple_of((x >> 1) * 512 + c * 256 + y * 64, 64)
            block = piece[dx].astype(jnp.int32)
            step = step_of(block[:, 512:513], block[:, 513:514])
            held[number, dx] = block[:, :512].astype(f32) * step
            copies.append(
                pltpu.make_async_copy(
                    held.at[number, dx], out_ref.at[pl.ds(top, 64), pl.ds(left, 512)], sems.at[number, dx]
                )
            )
            copies[-1].start()
    for copy in copies:
        copy.wait()


def placed(at, pieces):
    return pl.pallas_call(
        place_kernel,
        in_specs=[pl.BlockSpec(memory_space=pltpu.SMEM)] + [pl.BlockSpec(memory_space=pltpu.VMEM)] * len(pieces),
        out_specs=pl.BlockSpec(memory_space=pl.ANY),
        out_shape=jax.ShapeDtypeStruct((1024, 1024), f32),
        scratch_shapes=[
            pltpu.VMEM((2 * ring, ring, 64, 512), f32),
            pltpu.SemaphoreType.DMA((2 * ring, ring)),
        ],
        cost_estimate=pl.CostEstimate(flops=3 << 20, bytes_accessed=8 << 20, transcendentals=0),
        compiler_params=pltpu.CompilerParams(vmem_limit_bytes=12 << 20),
        name="place",
    )(at, *pieces)


def share_kernel(at_ref, left_ref, right_ref, *out_refs):
    for step, out_ref in enumerate(out_refs):
        of = (at_ref[0] + step) & 3
        out_ref[:, :512] = left_ref[:, pl.ds(pl.multiple_of((of >> 1) * 512, 512), 512)]
        out_ref[:, 512:] = right_ref[:, pl.ds(pl.multiple_of((of & 1) * 512, 512), 512)]


def shares(x, inputs, cotangents):
    return pl.pallas_call(
        share_kernel,
        in_specs=[pl.BlockSpec(memory_space=pltpu.SMEM)] + [pl.BlockSpec(memory_space=pltpu.VMEM)] * 2,
        out_shape=[jax.ShapeDtypeStruct(inputs.shape, bf16)] * ring,
        cost_estimate=pl.CostEstimate(flops=1 << 19, bytes_accessed=2 << 20, transcendentals=0),
        name="share",
    )(x[None], inputs, cotangents)


def gathered(value, axis):
    return [value] + [to_next(value, axis, step) for step in range(1, ring)]


def dense_sum(inputs, cotangents):
    y, x, c = (lax.axis_index(a) for a in ("y", "x", "c"))

    parts = shares(x.astype(jnp.int32), inputs, cotangents)
    parts = [parts[0]] + [to_next(parts[step], "x", step) for step in range(1, ring)]
    both = jnp.concatenate(parts, axis=0)
    local = lax.dot_general(both[:, :512], both[:, 512:], (((0,), (0,)), ((), ())), preferred_element_type=f32)
    halves = local.reshape(2, 256, 512)
    swap = [(0, 1), (1, 0)]
    other = lax.ppermute(lax.dynamic_index_in_dim(halves, 1 - c, 0, keepdims=False), "c", swap)
    total = lax.dynamic_index_in_dim(halves, c, 0, keepdims=False) + other
    total = scattered(total.reshape(ring, 64, 512), "y", y)
    ranks = gathered(total, deep)
    total = coded_sum(ranks)
    mine = gathered(jnp.stack(gathered(total, "x")), "y")
    theirs = [lax.ppermute(p, "c", swap) for p in mine]
    return placed(jnp.stack([y, x, c]).astype(jnp.int32), mine + theirs)


def update_kernel(at_ref, table_ref, accum_ref, prior_ref, grad_ref, *refs):
    out_ref, new_ref = refs[-2:]
    at = at_ref[0]
    accum = jnp.where(at == 0, accum_ref[0:1, :], accum_ref[1:2, :])
    for top in range(0, grad_ref.shape[0], 128):
        span = slice(top, top + 128)
        grad = grad_ref[span, :]
        before = jnp.broadcast_to(accum[:, span], (128, 128)).T
        after = before + jnp.mean(grad * grad, axis=1, keepdims=True)
        out_ref[0, span, :] = table_ref[0, span, :] - learn_rate * grad / jnp.sqrt(after)
        row = after.T[0:1, :]
        new_ref[0:1, span] = jnp.where(at == 0, row, prior_ref[0:1, span])
        new_ref[1:2, span] = jnp.where(at == 0, prior_ref[1:2, span], row)


def updated(at, table_rows, row_accum, prior, grad, before=()):
    tables, rows, width = table_rows.shape
    small = pl.BlockSpec((tables, rows), lambda i, b: (0, 0))
    return pl.pallas_call(
        update_kernel,
        grid_spec=pltpu.PrefetchScalarGridSpec(
            num_scalar_prefetch=1,
            grid=(1,),
            in_specs=[
                pl.BlockSpec((1, rows, width), lambda i, b: (b[0], 0, 0)),
                small,
                small,
                pl.BlockSpec((rows, width), lambda i, b: (0, 0)),
            ]
            + [pl.BlockSpec(memory_space=pl.ANY)] * len(before),
            out_specs=[pl.BlockSpec((1, rows, width), lambda i, b: (b[0], 0, 0)), small],
        ),
        out_shape=[jax.ShapeDtypeStruct(table_rows.shape, f32), jax.ShapeDtypeStruct(row_accum.shape, f32)],
        input_output_aliases={5: 0} if before else {},
        cost_estimate=pl.CostEstimate(flops=1 << 20, bytes_accessed=2 << 20, transcendentals=0),
        compiler_params=pltpu.CompilerParams(vmem_limit_bytes=8 << 20),
        name="update",
    )(at[None], table_rows, row_accum, prior, grad, *before)


def per_device(
    pooled_grad, bag_lengths, bag_rows, table_rows, row_accum, dense_input, dense_cotangent
):
    tables, rows = row_accum.shape
    dense_grad = dense_sum(dense_input, dense_cotangent)
    codes = slot_codes(bag_lengths, bag_rows)

    def exchanged(value):
        return lax.all_to_all(value, every, split_axis=0, concat_axis=0, tiled=True)

    near = packed(pooled_grad, 0, (codes,))
    late = packed(pooled_grad, 1)
    first = exchanged(near)
    second = exchanged(late)
    half = lax.axis_index("zl").astype(jnp.int32)
    early = summed(0, first, first, jnp.zeros((1,), jnp.int32), tables * rows)
    theirs = summed(1, first, second, ((1 - half) * rows)[None], rows, (early,))
    arrived = lax.ppermute(theirs, "zl", [(0, 1), (1, 0)])
    own = summed(1, first, second, (half * rows)[None], rows, (early,))
    part_rows, part_accum = updated(half, table_rows, row_accum, row_accum, own)
    new_rows, new_accum = updated(1 - half, table_rows, row_accum, part_accum, arrived, (part_rows,))
    return (new_rows, new_accum, dense_grad)


def solution(mesh):
    fine = Mesh(mesh.devices.reshape(4, 4, 2, 2, 2), every)
    samples = P(every)
    owned = P(("y", "x", "zh", "c"), "zl")
    return jax.shard_map(
        per_device,
        mesh=fine,
        in_specs=(samples, samples, samples, owned, owned, samples, samples),
        out_specs=(owned, owned, P()),
        check_vma=False,
    )
```

```python
import functools

import jax
import jax.numpy as jnp
from jax import lax
from jax.experimental import pallas as pl
from jax.experimental.pallas import tpu as pltpu
from jax.sharding import Mesh, PartitionSpec as P


learn_rate = 0.5
ring = 4
every = ("y", "x", "zh", "c", "zl")
deep = ("zh", "zl")
f32 = jnp.float32
bf16 = jnp.bfloat16


def sized(row):
    size = (128 + (row & 127)) << ((row >> 7) & 7)
    return jnp.where(row >= 1024, -size, size)


def slot_codes(row_ref, count_ref, out_ref):
    samples, slots, tables = row_ref.shape
    row = [row_ref[:, j, :] for j in range(slots)]
    active = [count_ref[...] > j for j in range(slots)]
    kinds = []
    for j in range(slots):
        first = active[j]
        for i in range(j):
            first = first & (row[i] != row[j])
        kinds.append(jnp.where(first, sized(row[j]), 0))
    for j in range(slots):
        weight = jnp.ones_like(row[j])
        for i in range(j + 1, slots):
            weight = weight + jnp.where(active[i] & (row[i] == row[j]), 1, 0)
        kinds.append(weight)
    kinds = [kind.astype(f32).T.astype(bf16) for kind in kinds]
    size = 16 * len(kinds)
    to = lax.broadcasted_iota(jnp.int32, (size, size), 0)
    of = lax.broadcasted_iota(jnp.int32, (size, size), 1)
    turn = jnp.where(((to & 7) == (of >> 4)) & ((to >> 3) == (of & 15)), 1.0, 0.0).astype(bf16)
    for top in range(0, tables, 16):
        block = jnp.concatenate([kind[top : top + 16, :] for kind in kinds], axis=0)
        turned = jnp.dot(turn, block, preferred_element_type=f32)
        out_ref[top : top + 16] = turned.reshape(16, len(kinds), samples).astype(bf16)


def pack_kernel(grad_ref, *refs):
    lookups = refs[:2] if len(refs) == 5 else ()
    out_ref, swap_ref, *code_refs = refs[len(lookups) :]
    samples, tables, width = grad_ref.shape
    at = pl.program_id(0)

    @pl.when(at == 0)
    def _():
        to = lax.broadcasted_iota(jnp.int32, swap_ref.shape, 0)
        of = lax.broadcasted_iota(jnp.int32, swap_ref.shape, 1)
        hit = ((to & 15) == (of >> 4)) & ((to >> 4) == (of & 15))
        swap_ref[...] = jnp.where(hit, 1.0, 0.0).astype(bf16)
        for code_ref in code_refs:
            slot_codes(*lookups, code_ref)

    for first in range(0, samples, 16):
        for top in range(0, tables, 16):
            block = grad_ref[first : first + 16, top : top + 16].reshape(256, width)
            turned = jnp.dot(swap_ref[...], block, preferred_element_type=f32)
            out_ref[top : top + 16, first : first + 16, :] = turned.astype(bf16).reshape(16, 16, width)
    for code_ref in code_refs:
        out_ref[:, samples : samples + 8, :] = code_ref[pl.ds(pl.multiple_of(at * tables, tables), tables)]


def packed(grads, part, lookups=()):
    start, stop = cut[part : part + 2]
    samples, tables, width = grads.shape
    count = stop - start
    height = count + (8 if lookups else 0)
    codes = [pltpu.VMEM((tables, 8, samples), bf16)] if lookups else []
    return pl.pallas_call(
        pack_kernel,
        grid=(tables // 64,),
        in_specs=[
            pl.BlockSpec((pl.Element(count), pl.Element(64), pl.Element(width)), lambda i: (start, i * 64, 0))
        ]
        + [pl.BlockSpec(a.shape, lambda i, n=a.ndim: (0,) * n) for a in lookups],
        out_specs=pl.BlockSpec((64, height, width), lambda i: (i, 0, 0)),
        out_shape=jax.ShapeDtypeStruct((tables, height, width), bf16),
        scratch_shapes=[pltpu.VMEM((256, 256), bf16)] + codes,
        cost_estimate=pl.CostEstimate(flops=2 * 256 * count * tables * width, bytes_accessed=4 << 20, transcendentals=0),
        name="pack",
    )(grads, *lookups)


cut = (0, 80, 128)
group = 32
stripe = 512


def sum_kernel(part, base_ref, info_ref, data_ref, *refs):
    out_ref, mine_ref = refs[-2], refs[-1]
    senders, samples, width = data_ref.shape
    rows = out_ref.shape[0]

    @pl.when(pl.program_id(0) == 0)
    def _():
        out_ref[...] = refs[0][...] if len(refs) == 3 else jnp.zeros_like(out_ref)
        mine_ref[...] = sized(base_ref[0] + lax.broadcasted_iota(jnp.int32, mine_ref.shape, 0)).astype(f32)

    zero = jnp.zeros((), bf16)
    here = slice(*cut[part : part + 2])
    for first in range(0, senders, group):
        infos = jnp.concatenate([info_ref[k][:, here] for k in range(first, first + group)], axis=1)
        infos = [infos[:, k : k + width] for k in range(0, group * samples, width)]
        values = jnp.concatenate([data_ref[k, 0:samples, :] for k in range(first, first + group)], axis=0)
        for top in range(0, rows, stripe):
            mine = mine_ref[top : top + stripe, :].astype(bf16)
            hots = []
            for info in infos:
                hot = jnp.where(mine == info[3:4], info[7:8], zero)
                for j in (2, 1, 0):
                    hot = jnp.where(mine == info[j : j + 1], info[4 + j : 5 + j], hot)
                hots.append(hot)
            out_ref[top : top + stripe, :] += jnp.dot(
                jnp.concatenate(hots, axis=1), values, preferred_element_type=f32
            )


def summed(part, first, data, base, rows, before=()):
    senders, _, width = data.shape
    samples = cut[part + 1] - cut[part]
    step = 64
    return pl.pallas_call(
        functools.partial(sum_kernel, part),
        grid_spec=pltpu.PrefetchScalarGridSpec(
            num_scalar_prefetch=1,
            grid=(senders // step,),
            in_specs=[
                pl.BlockSpec((step, 8, width), lambda i, b: (i, cut[1] // 8, 0)),
                pl.BlockSpec((step, samples, width), lambda i, b: (i, 0, 0)),
            ]
            + [pl.BlockSpec((rows, width), lambda i, b: (b[0] // rows, 0))] * len(before),
            out_specs=pl.BlockSpec((rows, width), lambda i, b: (0, 0)),
            scratch_shapes=[pltpu.VMEM((rows, width), f32)],
        ),
        out_shape=jax.ShapeDtypeStruct((rows, width), f32),
        cost_estimate=pl.CostEstimate(flops=2 * senders * samples * rows * width, bytes_accessed=3 << 20, transcendentals=0),
        name="sum_by_row",
    )(base, first, data, *before)


def to_next(value, axis, step):
    return lax.ppermute(value, axis, [(i, (i + step) % ring) for i in range(ring)])


def scattered(value, axis, here):
    arrived = [
        to_next(lax.dynamic_index_in_dim(value, (here + step) & 3, 0, keepdims=False), axis, step)
        for step in range(1, ring)
    ]
    own = lax.dynamic_index_in_dim(value, here, 0, keepdims=False)
    return own + arrived[0] + arrived[1] + arrived[2]


def step_of(power, factor):
    return jnp.exp2(power.astype(f32)) * (factor.astype(f32) * (1 / 32767 / 8192))


def code_kernel(*refs):
    out_ref = refs[-1]
    total = (refs[0][...] + refs[2][...]) + (refs[1][...] + refs[3][...])
    top = jnp.max(jnp.abs(total), axis=1, keepdims=True)
    power = jnp.clip(jnp.floor(jnp.log2(jnp.maximum(top, 1e-30))), -90.0, 90.0).astype(jnp.int32)
    factor = jnp.ceil(top * jnp.exp2(-power.astype(f32)) * 8192).astype(jnp.int32)
    factor = jnp.clip(factor, 0, 32767)
    step = step_of(power, factor)
    value = jnp.round(total * jnp.where(step > 0, 1 / step, 0.0))
    value = jnp.clip(value, -32767, 32767).astype(jnp.int32)
    lane = lax.broadcasted_iota(jnp.int32, (total.shape[0], 128), 1)
    out_ref[:, :512] = value.astype(jnp.int16)
    out_ref[:, 512:] = jnp.where(lane == 0, power, factor).astype(jnp.int16)


def coded_sum(ranks):
    return pl.pallas_call(
        code_kernel,
        out_shape=jax.ShapeDtypeStruct((64, 640), jnp.int16),
        cost_estimate=pl.CostEstimate(flops=1 << 20, bytes_accessed=1 << 20, transcendentals=0),
        compiler_params=pltpu.CompilerParams(vmem_limit_bytes=4 << 20),
        name="code_sum",
    )(*ranks)


def place_kernel(at_ref, *refs):
    pieces, out_ref, held, sems = refs[: 2 * ring], refs[-3], refs[-2], refs[-1]
    here_y, here_x, here_c = (at_ref[k] for k in range(3))
    copies = []
    for number, piece in enumerate(pieces):
        c = here_c if number < ring else 1 - here_c
        y = (here_y - number) & 3
        for dx in range(ring):
            x = (here_x - dx) & 3
            left = pl.multiple_of((x & 1) * 512, 512)
            top = pl.multiple_of((x >> 1) * 512 + c * 256 + y * 64, 64)
            block = piece[dx].astype(jnp.int32)
            step = step_of(block[:, 512:513], block[:, 513:514])
            held[number, dx] = block[:, :512].astype(f32) * step
            copies.append(
                pltpu.make_async_copy(
                    held.at[number, dx], out_ref.at[pl.ds(top, 64), pl.ds(left, 512)], sems.at[number, dx]
                )
            )
            copies[-1].start()
    for copy in copies:
        copy.wait()


def placed(at, pieces):
    return pl.pallas_call(
        place_kernel,
        in_specs=[pl.BlockSpec(memory_space=pltpu.SMEM)] + [pl.BlockSpec(memory_space=pltpu.VMEM)] * len(pieces),
        out_specs=pl.BlockSpec(memory_space=pl.ANY),
        out_shape=jax.ShapeDtypeStruct((1024, 1024), f32),
        scratch_shapes=[
            pltpu.VMEM((2 * ring, ring, 64, 512), f32),
            pltpu.SemaphoreType.DMA((2 * ring, ring)),
        ],
        cost_estimate=pl.CostEstimate(flops=3 << 20, bytes_accessed=8 << 20, transcendentals=0),
        compiler_params=pltpu.CompilerParams(vmem_limit_bytes=12 << 20),
        name="place",
    )(at, *pieces)


def share_kernel(at_ref, left_ref, right_ref, *out_refs):
    for step, out_ref in enumerate(out_refs):
        of = (at_ref[0] + step) & 3
        out_ref[:, :512] = left_ref[:, pl.ds(pl.multiple_of((of >> 1) * 512, 512), 512)]
        out_ref[:, 512:] = right_ref[:, pl.ds(pl.multiple_of((of & 1) * 512, 512), 512)]


def shares(x, inputs, cotangents):
    return pl.pallas_call(
        share_kernel,
        in_specs=[pl.BlockSpec(memory_space=pltpu.SMEM)] + [pl.BlockSpec(memory_space=pltpu.VMEM)] * 2,
        out_shape=[jax.ShapeDtypeStruct(inputs.shape, bf16)] * ring,
        cost_estimate=pl.CostEstimate(flops=1 << 19, bytes_accessed=2 << 20, transcendentals=0),
        name="share",
    )(x[None], inputs, cotangents)


def gathered(value, axis):
    return [value] + [to_next(value, axis, step) for step in range(1, ring)]


def dense_sum(inputs, cotangents):
    y, x, c = (lax.axis_index(a) for a in ("y", "x", "c"))

    parts = shares(x.astype(jnp.int32), inputs, cotangents)
    parts = [parts[0]] + [to_next(parts[step], "x", step) for step in range(1, ring)]
    both = jnp.concatenate(parts, axis=0)
    local = lax.dot_general(both[:, :512], both[:, 512:], (((0,), (0,)), ((), ())), preferred_element_type=f32)
    halves = local.reshape(2, 256, 512)
    swap = [(0, 1), (1, 0)]
    other = lax.ppermute(lax.dynamic_index_in_dim(halves, 1 - c, 0, keepdims=False), "c", swap)
    total = lax.dynamic_index_in_dim(halves, c, 0, keepdims=False) + other
    total = scattered(total.reshape(ring, 64, 512), "y", y)
    ranks = gathered(total, deep)
    total = coded_sum(ranks)
    mine = gathered(jnp.stack(gathered(total, "x")), "y")
    theirs = [lax.ppermute(p, "c", swap) for p in mine]
    return placed(jnp.stack([y, x, c]).astype(jnp.int32), mine + theirs)


def update_kernel(at_ref, table_ref, accum_ref, prior_ref, grad_ref, *refs):
    out_ref, new_ref = refs[-2:]
    at = at_ref[0]
    accum = jnp.where(at == 0, accum_ref[0:1, :], accum_ref[1:2, :])
    for top in range(0, grad_ref.shape[0], 128):
        span = slice(top, top + 128)
        grad = grad_ref[span, :]
        before = jnp.broadcast_to(accum[:, span], (128, 128)).T
        after = before + jnp.mean(grad * grad, axis=1, keepdims=True)
        out_ref[0, span, :] = table_ref[0, span, :] - learn_rate * grad / jnp.sqrt(after)
        row = after.T[0:1, :]
        new_ref[0:1, span] = jnp.where(at == 0, row, prior_ref[0:1, span])
        new_ref[1:2, span] = jnp.where(at == 0, prior_ref[1:2, span], row)


def updated(at, table_rows, row_accum, prior, grad, before=()):
    tables, rows, width = table_rows.shape
    small = pl.BlockSpec((tables, rows), lambda i, b: (0, 0))
    return pl.pallas_call(
        update_kernel,
        grid_spec=pltpu.PrefetchScalarGridSpec(
            num_scalar_prefetch=1,
            grid=(1,),
            in_specs=[
                pl.BlockSpec((1, rows, width), lambda i, b: (b[0], 0, 0)),
                small,
                small,
                pl.BlockSpec((rows, width), lambda i, b: (0, 0)),
            ]
            + [pl.BlockSpec(memory_space=pl.ANY)] * len(before),
            out_specs=[pl.BlockSpec((1, rows, width), lambda i, b: (b[0], 0, 0)), small],
        ),
        out_shape=[jax.ShapeDtypeStruct(table_rows.shape, f32), jax.ShapeDtypeStruct(row_accum.shape, f32)],
        input_output_aliases={5: 0} if before else {},
        cost_estimate=pl.CostEstimate(flops=1 << 20, bytes_accessed=2 << 20, transcendentals=0),
        compiler_params=pltpu.CompilerParams(vmem_limit_bytes=8 << 20),
        name="update",
    )(at[None], table_rows, row_accum, prior, grad, *before)


def per_device(
    pooled_grad, bag_lengths, bag_rows, table_rows, row_accum, dense_input, dense_cotangent
):
    tables, rows = row_accum.shape
    dense_grad = dense_sum(dense_input, dense_cotangent)
    looked = jnp.transpose(bag_rows, (0, 2, 1))

    def exchanged(value):
        return lax.all_to_all(value, every, split_axis=0, concat_axis=0, tiled=True)

    near = packed(pooled_grad, 0, (looked, bag_lengths))
    late = packed(pooled_grad, 1)
    first = exchanged(near)
    second = exchanged(late)
    half = lax.axis_index("zl").astype(jnp.int32)
    early = summed(0, first, first, jnp.zeros((1,), jnp.int32), tables * rows)
    theirs = summed(1, first, second, ((1 - half) * rows)[None], rows, (early,))
    arrived = lax.ppermute(theirs, "zl", [(0, 1), (1, 0)])
    own = summed(1, first, second, (half * rows)[None], rows, (early,))
    part_rows, part_accum = updated(half, table_rows, row_accum, row_accum, own)
    new_rows, new_accum = updated(1 - half, table_rows, row_accum, part_accum, arrived, (part_rows,))
    return (new_rows, new_accum, dense_grad)


def solution(mesh):
    fine = Mesh(mesh.devices.reshape(4, 4, 2, 2, 2), every)
    samples = P(every)
    owned = P(("y", "x", "zh", "c"), "zl")
    return jax.shard_map(
        per_device,
        mesh=fine,
        in_specs=(samples, samples, samples, owned, owned, samples, samples),
        out_specs=(owned, owned, P()),
        check_vma=False,
    )
```
